64 devices in a mesh: rep: 8 (over x, y, core), dp: 8 (over z).
Axes of the slice: x: 2, y: 2, z: 8, core: 2. Of those that a mesh axis runs over, the one named last changes fastest.
The devices are a block of a 4x4x8 slice.
Arguments:
- x: bfloat16 [64, 4096, 640], P(('rep', 'dp')), parts along dimension 0
- dy: bfloat16 [64, 4096, 640], P(('rep', 'dp')), parts along dimension 0
- w_gate: bfloat16 [2, 640, 1536], replicated
- w_up: bfloat16 [2, 640, 1536], replicated
- w_down: bfloat16 [2, 1536, 640], replicated
- m_w_gate: float32 [2, 640, 1536], replicated
- m_w_up: float32 [2, 640, 1536], replicated
- m_w_down: float32 [2, 1536, 640], replicated
- v_w_gate: float32 [2, 640, 1536], replicated
- v_w_up: float32 [2, 640, 1536], replicated
- v_w_down: float32 [2, 1536, 640], replicated
Outputs:
- output 1: bfloat16 [16, 640, 1536], P('rep'), parts along dimension 0
- output 2: bfloat16 [16, 640, 1536], P('rep'), parts along dimension 0
- output 3: bfloat16 [16, 1536, 640], P('rep'), parts along dimension 0
- output 4: float32 [16, 640, 1536], P('rep'), parts along dimension 0
- output 5: float32 [16, 640, 1536], P('rep'), parts along dimension 0
- output 6: float32 [16, 1536, 640], P('rep'), parts along dimension 0
- output 7: float32 [16, 640, 1536], P('rep'), parts along dimension 0
- output 8: float32 [16, 640, 1536], P('rep'), parts along dimension 0
- output 9: float32 [16, 1536, 640], P('rep'), parts along dimension 0
There are 8 independent parts. The reference program is written for one: setup_inputs(seed, part) draws one part's arguments, and reference() takes and returns one part's arrays. A program takes and returns all parts, laid end to end along the dimension named above; an argument that names none is the same for every part.
All inputs are finite; a program needn't handle non-finite values.
Results may differ from the reference program's by a relative error of at most 0.022.
Values are sent between devices in bfloat16 or wider.
A program may use at most 768 MiB of HBM per device.

```python
import jax
import jax.numpy as jnp
from jax import lax

SEQUENCES = 8
TOKENS = 4096
D = 640
FF = 1536
LAYERS = 2
NAMES = ("w_gate", "w_up", "w_down")
SHAPES = {"w_gate": (LAYERS, D, FF), "w_up": (LAYERS, D, FF), "w_down": (LAYERS, FF, D)}


def bump(key, n, height):
    away = (jnp.arange(n, dtype=jnp.int32) - jax.random.randint(key, (), 0, n, jnp.int32)) % n
    return jnp.where(away < n // 8, height, 1.0)


def together(key, own, strength):
    shared = jax.random.normal(key, own.shape[1:], jnp.float32)
    return (own + strength * shared) * lax.rsqrt(1 + strength * strength)


def setup_inputs(seed: int = 0, part: int = 0) -> dict:
    kx, kdy, ka, kb, kz, kf, kh, kl, *keys = jax.random.split(jax.random.key(seed), 8 + 3 * len(NAMES))
    kx, kdy, ka, kb = (jax.random.fold_in(k, part) for k in (kx, kdy, ka, kb))
    kw, km, kv = (keys[i::3] for i in range(3))
    shape = (SEQUENCES, TOKENS, D)
    much_x, much_dy = jax.random.uniform(kz, (2,), jnp.float32, 0.0, 1.0)
    loud = 2.0 ** jax.random.uniform(jax.random.fold_in(kz, 1), (), jnp.float32, -1.0, 2.0)
    layers = 2.0 ** jax.random.uniform(kl, (LAYERS, 1, 1), jnp.float32, -1.0, 1.0)
    x = together(ka, jax.random.normal(kx, shape, jnp.float32), much_x) * bump(kf, D, 4.0)
    dy = together(kb, jax.random.normal(kdy, shape, jnp.float32), much_dy)
    drawn = {"x": x.astype(jnp.bfloat16), "dy": (loud * dy * (SEQUENCES * TOKENS) ** -0.5).astype(jnp.bfloat16)}
    for key, name in zip(kw, NAMES, strict=True):
        w = jax.random.normal(key, SHAPES[name], jnp.float32) * SHAPES[name][1] ** -0.5
        drawn[name] = (w * {"w_gate": 1.0, "w_up": bump(kh, FF, 4.0), "w_down": layers}[name]).astype(jnp.bfloat16)
    for key, name in zip(km, NAMES, strict=True):
        drawn[f"m_{name}"] = 0.1 * jax.random.normal(key, SHAPES[name], jnp.float32)
    for key, name in zip(kv, NAMES, strict=True):
        drawn[f"v_{name}"] = jax.random.uniform(key, SHAPES[name], jnp.float32, 0.005, 0.015)
    return drawn


def matmul(a, w):
    return jnp.dot(a, w, preferred_element_type=jnp.float32).astype(jnp.bfloat16)


def normed(h):
    wide = h.astype(jnp.float32)
    scale = lax.rsqrt(jnp.mean(wide**2, -1, keepdims=True) + 1e-6)
    return (wide * scale).astype(jnp.bfloat16)


def layer(h, w):
    a = normed(h)
    gate = jnp.dot(a, w["w_gate"], preferred_element_type=jnp.float32)
    up = jnp.dot(a, w["w_up"], preferred_element_type=jnp.float32)
    return h + matmul((jax.nn.silu(gate) * up).astype(jnp.bfloat16), w["w_down"])


def adamw(w, m, v, g):
    m = 0.9 * m + 0.1 * g
    v = 0.95 * v + 0.05 * g * g
    step = m * lax.rsqrt(v + 1e-8) + 0.1 * w
    return (w - 0.02 * step).astype(jnp.bfloat16), m, v


def clipped(gradients, sum_of_squares, count):
    factor = jnp.minimum(1.0, 0.5 * lax.rsqrt(sum_of_squares / count + 1e-30))
    return [g * factor for g in gradients]


def stack(weights, h):
    return lax.scan(lambda h, w: (layer(h, w), None), h, weights)[0]


def reference(x, dy, w_gate, w_up, w_down, m_w_gate, m_w_up, m_w_down, v_w_gate, v_w_up, v_w_down):
    weights = dict(zip(NAMES, (w_gate, w_up, w_down), strict=True))

    def take(so_far, sequence):
        h, by_y = sequence
        _, back = jax.vjp(lambda w: stack(w, h), weights)
        return jax.tree.map(lambda total, term: total + term.astype(jnp.float32), so_far, back(by_y)[0]), None

    none_yet = {name: jnp.zeros(w.shape, jnp.float32) for name, w in weights.items()}
    by_weights, _ = lax.scan(take, none_yet, (x, dy))
    gradients = [by_weights[name].astype(jnp.bfloat16).astype(jnp.float32) for name in NAMES]
    gradients = clipped(gradients, sum(jnp.sum(g * g) for g in gradients), sum(g.size for g in gradients))
    new = [
        adamw(w.astype(jnp.float32), m, v, g)
        for w, m, v, g in zip((w_gate, w_up, w_down), (m_w_gate, m_w_up, m_w_down), (v_w_gate, v_w_up, v_w_down), gradients, strict=True)
    ]
    return tuple(one[which] for which in range(3) for one in new)
```

```python
import functools

import jax
import jax.numpy as jnp
from jax import lax
from jax.experimental import pallas as pl
from jax.experimental.pallas import tpu as pltpu
from jax.sharding import PartitionSpec as P

BF16, F32 = jnp.bfloat16, jnp.float32
MESH = pl.DeviceIdType.MESH
LANES = 128
FORWARD_TILE, TILE, BLOCK = 512, 1024, 256
PLAIN, BY_ROWS = ((1,), (0,)), ((1,), (1,))


def dot(a, b, contract=PLAIN):
    return lax.dot_general(a, b, (contract, ((), ())), preferred_element_type=F32)


def scale_of(wide):
    return lax.rsqrt(jnp.mean(wide * wide, -1, keepdims=True) + 1e-6)


def normed(h):
    wide = h.astype(F32)
    return (wide * scale_of(wide)).astype(BF16)


def forward_kernel(x_ref, dy_ref, wg_ref, wu_ref, wd_ref, h_ref, a0_ref, a0t_ref, a1_ref, a1t_ref, dyt_ref):
    x = x_ref[...]
    a0 = normed(x)
    a0_ref[...] = a0
    a0t_ref[...] = a0.T
    dyt_ref[...] = dy_ref[...].T
    gate = dot(a0, wg_ref[...])
    up = dot(a0, wu_ref[...])
    z = (gate * jax.nn.sigmoid(gate) * up).astype(BF16)
    h = (x.astype(F32) + dot(z, wd_ref[...]).astype(BF16).astype(F32)).astype(BF16)
    h_ref[...] = h
    a1 = normed(h)
    a1_ref[...] = a1
    a1t_ref[...] = a1.T


def forward(x, dy, w_gate, w_up, w_down):
    tokens, d = x.shape[1:]
    ff = w_gate.shape[2]
    tile = min(FORWARD_TILE, tokens)
    rows = pl.BlockSpec((tile, d), lambda i: (i, 0))
    turned = pl.BlockSpec((d, tile), lambda i: (0, i))
    given = pl.BlockSpec((None, tile, d), lambda i: (0, i, 0))
    wide, tall = jax.ShapeDtypeStruct((tokens, d), BF16), jax.ShapeDtypeStruct((d, tokens), BF16)
    return pl.pallas_call(
        forward_kernel,
        grid=(tokens // tile,),
        in_specs=[given, given]
        + [pl.BlockSpec((None, d, ff), lambda i: (0, 0, 0))] * 2
        + [pl.BlockSpec((None, ff, d), lambda i: (0, 0, 0))],
        out_specs=[rows, rows, turned, rows, turned, turned],
        out_shape=[wide, wide, tall, wide, tall, tall],
        compiler_params=pltpu.CompilerParams(vmem_limit_bytes=63 << 20),
        cost_estimate=pl.CostEstimate(flops=6 * tokens * d * ff, bytes_accessed=16 * tokens * d, transcendentals=tokens * ff),
        name="forward",
    )(x, dy, w_gate, w_up, w_down)


def when(condition, do):
    if isinstance(condition, bool):
        if condition:
            do()
    else:
        pl.when(condition)(do)


def main_kernel(
    n, h_hbm, a0_hbm, a0t_hbm, a1_hbm, a1t_hbm, dy_hbm, dyt_hbm, wg_hbm, wu_hbm, wd_hbm,
    g1_ref, g0_ref, total_ref,
    a, at, g, gt, da, hbuf, wgu, wd, acc_gu, acc_d, own, from_left, from_right, squares, parts,
    in_sem, w_sem, h_sem, send_sem, recv_sem, part_send, part_recv, credit,
):
    tokens, d = a.shape
    block = wd.shape[1]
    blocks = wg_hbm.shape[2] // block
    units, half = 2 * blocks, n // 2
    tile = hbuf.shape[1]
    tiles = tokens // tile
    slots, shard_rows = own.shape[0], own.shape[2]
    me = lax.axis_index("dp")
    right, left = lax.rem(me + 1, n), lax.rem(me + n - 1, n)

    def loads(t, first, second):
        rows = pl.ds(pl.multiple_of(t * tile, tile), tile)
        return [
            pltpu.make_async_copy(first.at[rows], a.at[rows], in_sem.at[0, t]),
            pltpu.make_async_copy(second.at[:, rows], at.at[:, rows], in_sem.at[1, t]),
        ]

    def gradient_loads(t):
        rows = pl.ds(pl.multiple_of(t * tile, tile), tile)
        return [
            pltpu.make_async_copy(dy_hbm.at[rows], g.at[rows], in_sem.at[2, t]),
            pltpu.make_async_copy(dyt_hbm.at[:, rows], gt.at[:, rows], in_sem.at[3, t]),
        ]

    def weight_loads(b):
        last = jnp.int32(b < blocks) if isinstance(b, int) else (b < blocks).astype(jnp.int32)
        columns = pl.ds(pl.multiple_of((b - blocks * (1 - last)) * block, block), block)
        slot = lax.rem(b, 2)
        return [
            pltpu.make_async_copy(wg_hbm.at[last, :, columns], wgu.at[slot, :, pl.ds(0, block)], w_sem.at[0, slot]),
            pltpu.make_async_copy(wu_hbm.at[last, :, columns], wgu.at[slot, :, pl.ds(block, block)], w_sem.at[1, slot]),
            pltpu.make_async_copy(wd_hbm.at[last, columns, :], wd.at[slot], w_sem.at[2, slot]),
        ]

    def state_load(t):
        rows = pl.ds(pl.multiple_of(t * tile, tile), tile)
        slot = lax.rem(t, 2)
        return pltpu.make_async_copy(h_hbm.at[rows], hbuf.at[slot], h_sem.at[slot])

    def ring_copy(u, k, way):
        slot = lax.rem(u, slots)
        ahead = half - k if way == 0 else n - half + k
        shard = lax.rem(me + ahead, n)
        rows = pl.ds(0, shard_rows)
        if k == 0:
            rows = pl.ds(way * (shard_rows // 2), shard_rows // 2)
        return pltpu.make_async_remote_copy(
            src_ref=own.at[slot, shard, rows],
            dst_ref=(from_left, from_right)[way].at[slot, k, rows],
            send_sem=send_sem.at[way, slot, k],
            recv_sem=recv_sem.at[way, slot, k],
            device_id={"dp": (right, left)[way]},
            device_id_type=MESH,
        )

    def event(u, e):
        slot = lax.rem(u, slots)
        if e == 0:

            def take():
                pl.semaphore_wait(credit.at[0], 1)
                pl.semaphore_wait(credit.at[1], 1)

            when(u >= slots, take)
        else:
            for way in (0, 1):
                ring_copy(u, e - 1, way).wait()
        if 0 < e < half:
            for way in (0, 1):
                shard = lax.rem(me + (half - e if way == 0 else n - half + e), n)
                rows = pl.ds(0, shard_rows) if e > 1 else pl.ds(way * (shard_rows // 2), shard_rows // 2)
                came = (from_left, from_right)[way][slot, e - 1, rows].astype(F32)
                own[slot, shard, rows] = (own[slot, shard, rows].astype(F32) + came).astype(BF16)
        if e < half:
            for way in (0, 1):
                ring_copy(u, e, way).start()
        else:
            came = from_left[slot, e - 1].astype(F32) + from_right[slot, e - 1].astype(F32)
            done = (own[slot, me].astype(F32) + came).astype(BF16)

            def keep(ref, index):
                def do():
                    ref[index] = done

                return do

            when(u < blocks, keep(g1_ref, jnp.minimum(u, blocks - 1)))
            when(u >= blocks, keep(g0_ref, jnp.maximum(u - blocks, 0)))
            wide = done.astype(F32)
            squares[...] += jnp.sum((wide * wide).reshape(shard_rows // 8, 8, LANES), 0)

            def give():
                pl.semaphore_signal(credit.at[0], 1, device_id={"dp": left}, device_id_type=MESH)
                pl.semaphore_signal(credit.at[1], 1, device_id={"dp": right}, device_id_type=MESH)

            when(u < units - slots, give)

    def events(b, t):
        for e in range(half + 1):
            lag, at_tile = divmod(5 * e // 2, tiles)
            u = b - 1 - lag
            if isinstance(b, int):
                if t == at_tile and 0 <= u < units:
                    event(u, e)
            else:

                @pl.when((t == at_tile) & (u >= 0))
                def _(u=u, e=e):
                    event(u, e)

    def steps(b, t, last):
        rows = pl.ds(pl.multiple_of(t * tile, tile), tile)
        slot = lax.rem(b, 2)
        gu = dot(a[rows], wgu[slot])
        dz = dot(g[rows], wd[slot], BY_ROWS).astype(BF16).astype(F32)
        gate, up = gu[:, :block], gu[:, block:]
        s = jax.nn.sigmoid(gate)
        silu = gate * s
        z = (silu * up).astype(BF16)
        dgate = (dz * up * (s + silu * (1 - s))).astype(BF16)
        dup = (dz * silu).astype(BF16)
        dgu = jnp.concatenate([dgate, dup], 1)
        acc_d[...] += dot(gt[:, rows], z)
        acc_gu[...] += dot(at[:, rows], dgu)
        if last:
            da[rows] += dot(dgu, wgu[slot], BY_ROWS)

    def pack(b):
        slot = lax.rem(b, slots)
        of_d, of_block = d // n, block // n
        for s in range(n):
            for c in range(2 * block // LANES):
                piece = acc_gu[pl.ds(s * of_d, of_d), pl.ds(c * LANES, LANES)]
                own[slot, s, pl.ds(c * of_d, of_d)] = piece.astype(BF16)
        base = 2 * block // LANES * of_d
        for c in range(d // LANES):
            turned = acc_d[pl.ds(c * LANES, LANES)].T.astype(BF16)
            for s in range(n):
                own[slot, s, pl.ds(base + c * of_block, of_block)] = turned[s * of_block : (s + 1) * of_block]

    def one_block(b, last):
        @pl.when(b + 1 < units)
        def _():
            for copy in weight_loads(b + 1):
                copy.start()

        for copy in weight_loads(b):
            copy.wait()
        acc_gu[...] = jnp.zeros_like(acc_gu)
        acc_d[...] = jnp.zeros_like(acc_d)

        @pl.loop(0, tiles)
        def _(t):
            @pl.when(b == (0 if last else blocks))
            def _():
                for copy in loads(t, a1_hbm, a1t_hbm) if last else loads(t, a0_hbm, a0t_hbm):
                    copy.wait()
                if last:
                    for copy in gradient_loads(t):
                        copy.wait()

            steps(b, t, last)
            if last:

                @pl.when(b == blocks - 1)
                def _():
                    for copy in loads(t, a0_hbm, a0t_hbm):
                        copy.start()

            events(b, t)

        pack(b)

    for t in range(tiles):
        for copy in loads(t, a1_hbm, a1t_hbm) + gradient_loads(t):
            copy.start()
        if t == 0:
            for copy in weight_loads(0):
                copy.start()
    for t in range(min(2, tiles)):
        state_load(t).start()
    barrier = pltpu.get_barrier_semaphore()
    for k in range(1, n):
        pl.semaphore_signal(barrier, 1, device_id={"dp": lax.rem(me + k, n)}, device_id_type=MESH)
    squares[...] = jnp.zeros_like(squares)

    @pl.loop(0, tiles)
    def _(t):
        da[pl.ds(pl.multiple_of(t * tile, tile), tile)] = jnp.zeros((tile, d), F32)

    pl.semaphore_wait(barrier, n - 1)

    @pl.loop(0, blocks)
    def _(b):
        one_block(b, True)

    @pl.loop(0, tiles)
    def _(t):
        state_load(t).wait()
        slot = lax.rem(t, 2)
        part = min(256, tile)

        @pl.loop(0, tile // part)
        def _(i):
            inner = pl.ds(pl.multiple_of(i * part, part), part)
            rows = pl.ds(pl.multiple_of(t * tile + i * part, part), part)
            wide = hbuf[slot, inner].astype(F32)
            scale = scale_of(wide)
            by_a = da[rows].astype(BF16).astype(F32)
            along = jnp.mean(by_a * wide, -1, keepdims=True)
            by_h = (by_a * scale - wide * (scale * scale * scale * along)).astype(BF16)
            out = (g[rows].astype(F32) + by_h.astype(F32)).astype(BF16)
            g[rows] = out
            gt[:, rows] = out.T

        @pl.when(t + 2 < tiles)
        def _():
            state_load(t + 2).start()

    @pl.loop(blocks, units)
    def _(b):
        one_block(b, False)

    for b in range(units, units + 1 + (5 * half // 2) // tiles):
        for t in range(tiles):
            events(b, t)

    def part_copy(k):
        return pltpu.make_async_remote_copy(
            src_ref=squares,
            dst_ref=parts.at[me],
            send_sem=part_send.at[k - 1],
            recv_sem=part_recv.at[k - 1],
            device_id={"dp": lax.rem(me + k, n)},
            device_id_type=MESH,
        )

    for k in range(1, n):
        part_copy(k).start()
    parts[me] = squares[...]
    for k in range(1, n):
        part_copy(k).wait()
    total = parts[0]
    for k in range(1, n):
        total = total + parts[k]
    total_ref[...] = total


def reduced(n, h, a0, a0t, a1, a1t, dy, dyt, w_gate, w_up, w_down):
    tokens, d = h.shape
    ff = w_gate.shape[2]
    block, tile = BLOCK, min(TILE, tokens // 4)
    tiles, blocks, half = tokens // tile, ff // block, n // 2
    shard_rows = 3 * d * block // (n * LANES)
    slots = (5 * half // 2) // tiles + 2
    shard = jax.ShapeDtypeStruct((blocks, shard_rows, LANES), BF16)
    anywhere, vmem = pl.BlockSpec(memory_space=pl.ANY), pl.BlockSpec(memory_space=pltpu.VMEM)
    return pl.pallas_call(
        functools.partial(main_kernel, n),
        in_specs=[anywhere] * 10,
        out_specs=[vmem] * 3,
        out_shape=[shard, shard, jax.ShapeDtypeStruct((8, LANES), F32)],
        scratch_shapes=[
            pltpu.VMEM((tokens, d), BF16),
            pltpu.VMEM((d, tokens), BF16),
            pltpu.VMEM((tokens, d), BF16),
            pltpu.VMEM((d, tokens), BF16),
            pltpu.VMEM((tokens, d), F32),
            pltpu.VMEM((2, tile, d), BF16),
            pltpu.VMEM((2, d, 2 * block), BF16),
            pltpu.VMEM((2, block, d), BF16),
            pltpu.VMEM((d, 2 * block), F32),
            pltpu.VMEM((d, block), F32),
            pltpu.VMEM((slots, n, shard_rows, LANES), BF16),
            pltpu.VMEM((slots, half, shard_rows, LANES), BF16),
            pltpu.VMEM((slots, half, shard_rows, LANES), BF16),
            pltpu.VMEM((8, LANES), F32),
            pltpu.VMEM((n, 8, LANES), F32),
            pltpu.SemaphoreType.DMA((4, tiles)),
            pltpu.SemaphoreType.DMA((3, 2)),
            pltpu.SemaphoreType.DMA((2,)),
            pltpu.SemaphoreType.DMA((2, slots, half)),
            pltpu.SemaphoreType.DMA((2, slots, half)),
            pltpu.SemaphoreType.DMA((n - 1,)),
            pltpu.SemaphoreType.DMA((n - 1,)),
            pltpu.SemaphoreType.REGULAR((2,)),
        ],
        compiler_params=pltpu.CompilerParams(collective_id=0, has_side_effects=True, vmem_limit_bytes=63 << 20),
        cost_estimate=pl.CostEstimate(flops=28 * tokens * d * ff, bytes_accessed=16 * tokens * d, transcendentals=2 * tokens * ff),
        name="reduced",
    )(h, a0, a0t, a1, a1t, dy, dyt, w_gate, w_up, w_down)


def update_kernel(count, n_terms, n_aliased, shards, total_ref, *refs):
    terms, refs = refs[:n_terms], refs[n_terms:]
    w, m, v = refs[:3], refs[3:6], refs[6:9]
    new_w, new_m, new_v = (refs[9 + n_aliased + 3 * i : 12 + n_aliased + 3 * i] for i in range(3))
    factor = jnp.minimum(1.0, 0.5 * lax.rsqrt(jnp.sum(total_ref[...], keepdims=True) / count + 1e-30))

    def apply(units, take):
        of_d, block = w[0].shape[0], w[0].shape[1] // units
        of_block, d = w[2].shape[1:]
        slabs = block // LANES

        def one(i, where, term):
            term = term.astype(F32) * factor
            m_new = 0.9 * m[i][where] + 0.1 * term
            v_new = 0.95 * v[i][where] + 0.05 * term * term
            wide = w[i][where].astype(F32)
            new_m[i][where] = m_new
            new_v[i][where] = v_new
            new_w[i][where] = (wide - 0.02 * (m_new * lax.rsqrt(v_new + 1e-8) + 0.1 * wide)).astype(BF16)

        for j in range(units):
            for i in range(2):
                for c in range(slabs):
                    row = (i * slabs + c) * of_d
                    one(i, (slice(None), pl.ds(j * block + c * LANES, LANES)), take(j, row, of_d))
            for c in range(d // LANES):
                one(2, (j, slice(None), pl.ds(c * LANES, LANES)), take(j, 2 * slabs * of_d + c * of_block, of_block))

    units, rows = terms[0].shape[:2]

    def from_one(ref):
        return lambda j, row, size: ref[j, pl.ds(row, size)]

    def from_halves(j, row, size):
        if row + size <= rows:
            return terms[0][j, pl.ds(row, size)]
        if row >= rows:
            return terms[1][j, pl.ds(row - rows, size)]
        first = rows - row
        return jnp.concatenate([terms[0][j, pl.ds(row, first)], terms[1][j, pl.ds(0, size - first)]], 0)

    full = (2 * w[0].shape[1] * w[0].shape[0] + units * w[2].shape[1] * w[2].shape[2]) // (units * LANES)
    if rows < full:
        apply(units, from_halves)
    elif n_terms == 1:
        apply(units, from_one(terms[0]))
    else:
        for i in range(n_terms):

            @pl.when(pl.program_id(0) == i)
            def _(i=i):
                apply(units, from_one(terms[i]))


def update(layer, shards, terms, total, weights, m, v, so_far):
    _, d, ff = weights[0].shape
    _, blocks, n, of_block, _ = weights[2].shape
    cut = 2
    of_d = d // n
    flat = pl.BlockSpec((None, of_d, ff // cut), lambda i, c, shards: (layer, shards[i], c))
    tall = pl.BlockSpec((None, blocks // cut, None, of_block, d), lambda i, c, shards: (layer, c, shards[i], 0, 0))
    term = pl.BlockSpec((blocks // cut, *terms[0].shape[1:]), lambda i, c, shards: (c, 0, 0))
    arrays = [*weights, *m, *v]
    specs = [flat, flat, tall] * 3
    aliased = list(so_far) if so_far is not None else []
    first = 2 + len(terms) + len(arrays)
    n_shards = shards.shape[0]
    bytes_accessed = n_shards * 20 * 3 * d * ff // n
    return pl.pallas_call(
        functools.partial(update_kernel, 3 * weights[0].size, len(terms), len(aliased)),
        grid_spec=pltpu.PrefetchScalarGridSpec(
            num_scalar_prefetch=1,
            grid=(n_shards, cut),
            in_specs=[pl.BlockSpec((8, LANES), lambda i, c, shards: (0, 0))]
            + [term] * len(terms)
            + specs
            + [pl.BlockSpec(memory_space=pl.ANY)] * len(aliased),
            out_specs=specs,
        ),
        out_shape=[jax.ShapeDtypeStruct(one.shape, one.dtype) for one in arrays],
        input_output_aliases={first + i: i for i in range(len(aliased))},
        compiler_params=pltpu.CompilerParams(vmem_limit_bytes=63 << 20),
        cost_estimate=pl.CostEstimate(flops=300 * bytes_accessed, bytes_accessed=bytes_accessed, transcendentals=0),
        name=f"update_{layer}",
    )(shards, total, *terms, *arrays, *aliased)


def solution(mesh):
    n = mesh.shape["dp"]
    half = n // 2

    def step(x, dy, *arrays):
        weights, m, v = (list(arrays[i : i + 3]) for i in (0, 3, 6))
        h, a0, a0t, a1, a1t, dyt = forward(x, dy, *weights)
        g1, g0, total = reduced(n, h, a0, a0t, a1, a1t, dy[0], dyt, *weights)

        layers, ff, d = weights[2].shape
        split = (layers, ff // BLOCK, n, BLOCK // n, d)
        for group in (weights, m, v):
            group[2] = group[2].reshape(split)
        me = lax.axis_index("dp")

        def sent(value, by):
            return lax.ppermute(value, "dp", [(i, (i + by) % n) for i in range(n)])

        rows = g1.shape[1]
        out = None
        came = {1: [(g1, g1)], 0: [(g0, g0)]}
        for k in range(half + 1):
            for layer in (1, 0):
                if k:
                    rightward, leftward = came[layer][-1]
                    if k == half:
                        rightward, leftward = rightward[:, : rows // 2], leftward[:, rows // 2 :]
                    came[layer].append((sent(rightward, 1), sent(leftward, -1)))
        for k in range(half + 1):
            for layer in (1, 0):
                terms = came[layer][k][:1] if k == 0 else came[layer][k]
                places = [me - k] if k in (0, half) else [me - k, me + k]
                shards = jnp.stack([lax.rem(place + n, n) for place in places]).astype(jnp.int32)
                out = update(layer, shards, terms, total, weights, m, v, out)
        out = list(out)
        for i in (2, 5, 8):
            out[i] = out[i].reshape(layers, ff, d)
        return tuple(out)

    return jax.shard_map(
        step,
        mesh=mesh,
        in_specs=(P(("rep", "dp"), None, None),) * 2 + (P(None, None, None),) * 9,
        out_specs=(P("rep", None, None),) * 9,
        check_vma=False,
    )
```

```python
import functools

import jax
import jax.numpy as jnp
from jax import lax
from jax.experimental import pallas as pl
from jax.experimental.pallas import tpu as pltpu
from jax.sharding import PartitionSpec as P

BF16, F32 = jnp.bfloat16, jnp.float32
MESH = pl.DeviceIdType.MESH
LANES = 128
BLOCK = 256
PLAIN, BY_ROWS = ((1,), (0,)), ((1,), (1,))


def dot(a, b, contract=PLAIN):
    return lax.dot_general(a, b, (contract, ((), ())), preferred_element_type=F32)


def scale_of(wide):
    return lax.rsqrt(jnp.mean(wide * wide, -1, keepdims=True) + 1e-6)


def normed(h):
    wide = h.astype(F32)
    return (wide * scale_of(wide)).astype(BF16)


def when(condition, do):
    if isinstance(condition, bool):
        if condition:
            do()
    else:
        pl.when(condition)(do)


def at_ring(e):
    return 5 * e // 2


def at_gather(e, half):
    return at_ring(half) + (3 + 4 * e if e else 0)


def main_kernel(
    n, x_hbm, dy_hbm, wg_hbm, wu_hbm, wd_hbm,
    g1_hbm, g0a_ref, g0b_ref, total_ref, a0_hbm, a0t_hbm, h_hbm, dgu_hbm,
    a, at, g, gt, wide, wgu, wd, acc_gu, acc_d, dgu, own, from_left, from_right, kept, squares, parts,
    x_sem, dy_sem, wide_sem, w_sem, dgu_sem, in_sem, send_sem, recv_sem, there_sem, here_sem, kept_sem, part_send, part_recv, credit,
):
    tokens, d = a.shape
    ff = wg_hbm.shape[2]
    block = wd.shape[1]
    blocks = ff // block
    units, half = 2 * blocks, n // 2
    tile = dgu.shape[1]
    tiles = tokens // tile
    small = tile // 2
    smalls = tokens // small
    slots, shard_rows = own.shape[0], own.shape[2]
    me = lax.axis_index("dp")
    right, left = lax.rem(me + 1, n), lax.rem(me + n - 1, n)

    def span(i, size):
        return pl.ds(i * size, size) if isinstance(i, int) else pl.ds(pl.multiple_of(i * size, size), size)

    def dy_load(i):
        return pltpu.make_async_copy(dy_hbm.at[0, span(i, small)], g.at[span(i, small)], dy_sem.at[i])

    def wide_loads(layer):
        return [
            pltpu.make_async_copy(wg_hbm.at[layer], wide.at[:, pl.ds(0, ff)], wide_sem.at[0]),
            pltpu.make_async_copy(wu_hbm.at[layer], wide.at[:, pl.ds(ff, ff)], wide_sem.at[1]),
        ]

    def a0_loads(t):
        return [
            pltpu.make_async_copy(a0_hbm.at[span(t, tile)], a.at[span(t, tile)], in_sem.at[0, t]),
            pltpu.make_async_copy(a0t_hbm.at[:, span(t, tile)], at.at[:, span(t, tile)], in_sem.at[1, t]),
        ]

    def weight_loads(b):
        last = jnp.int32(b < blocks) if isinstance(b, int) else (b < blocks).astype(jnp.int32)
        columns = pl.ds(pl.multiple_of((b - blocks * (1 - last)) * block, block), block)
        slot = lax.rem(b, 2)
        return [
            pltpu.make_async_copy(wg_hbm.at[last, :, columns], wgu.at[slot, :, pl.ds(0, block)], w_sem.at[0, slot]),
            pltpu.make_async_copy(wu_hbm.at[last, :, columns], wgu.at[slot, :, pl.ds(block, block)], w_sem.at[1, slot]),
            pltpu.make_async_copy(wd_hbm.at[last, columns, :], wd.at[slot], w_sem.at[2, slot]),
        ]

    def ring_copy(u, k, way):
        slot = lax.rem(u, slots)
        ahead = half - k if way == 0 else n - half + k
        shard = lax.rem(me + ahead, n)
        rows = pl.ds(0, shard_rows)
        if k == 0:
            rows = pl.ds(way * (shard_rows // 2), shard_rows // 2)
        return pltpu.make_async_remote_copy(
            src_ref=own.at[slot, shard, rows],
            dst_ref=(from_left, from_right)[way].at[slot, k, rows],
            send_sem=send_sem.at[way, slot, k],
            recv_sem=recv_sem.at[way, slot, k],
            device_id={"dp": (right, left)[way]},
            device_id_type=MESH,
        )

    def ring_event(u, e, last):
        slot = lax.rem(u, slots)
        if e == 0:

            def take():
                pl.semaphore_wait(credit.at[0], 1)
                pl.semaphore_wait(credit.at[1], 1)

            when(u >= slots, take)
        else:
            for way in (0, 1):
                ring_copy(u, e - 1, way).wait()
        if 0 < e < half:
            for way in (0, 1):
                shard = lax.rem(me + (half - e if way == 0 else n - half + e), n)
                rows = pl.ds(0, shard_rows) if e > 1 else pl.ds(way * (shard_rows // 2), shard_rows // 2)
                came = (from_left, from_right)[way][slot, e - 1, rows].astype(F32)
                own[slot, shard, rows] = (own[slot, shard, rows].astype(F32) + came).astype(BF16)
        if e < half:
            for way in (0, 1):
                ring_copy(u, e, way).start()
        else:
            came = from_left[slot, e - 1].astype(F32) + from_right[slot, e - 1].astype(F32)
            done = (own[slot, me].astype(F32) + came).astype(BF16)
            if last:
                kept[u] = done
            else:

                def keep(ref, place):
                    def do():
                        ref[place] = done

                    return do

                cut = blocks + blocks // 2
                when(u < cut, keep(g0a_ref, jnp.minimum(u - blocks, blocks // 2 - 1)))
                when(u >= cut, keep(g0b_ref, jnp.maximum(u - cut, 0)))
            exact = done.astype(F32)
            squares[...] += jnp.sum((exact * exact).reshape(shard_rows // 8, 8, LANES), 0)

            def give():
                pl.semaphore_signal(credit.at[0], 1, device_id={"dp": left}, device_id_type=MESH)
                pl.semaphore_signal(credit.at[1], 1, device_id={"dp": right}, device_id_type=MESH)

            when(u < units - slots, give)

    def gather_copy(u, k, way):
        rows = pl.ds(0, shard_rows)
        if k == half - 1:
            rows = pl.ds(way * (shard_rows // 2), shard_rows // 2)
        place = (k, n - k)[way]
        after = (k + 1, n - k - 1)[way]
        return pltpu.make_async_remote_copy(
            src_ref=kept.at[u, rows] if k == 0 else g1_hbm.at[place, u, rows],
            dst_ref=g1_hbm.at[after, u, rows],
            send_sem=there_sem.at[way, u, k],
            recv_sem=here_sem.at[way, u, k],
            device_id={"dp": (right, left)[way]},
            device_id_type=MESH,
        )

    def kept_copy(u):
        return pltpu.make_async_copy(kept.at[u], g1_hbm.at[0, u], kept_sem.at[u])

    def gather_event(u, e):
        if e == 0:
            kept_copy(u).start()
        else:
            for way in (0, 1):
                gather_copy(u, e - 1, way).wait()
        if e < half:
            for way in (0, 1):
                gather_copy(u, e, way).start()
        else:
            kept_copy(u).wait()

    between = tiles * blocks
    second = between + smalls

    def events(now, phase):
        for last in (True, False):
            base, first = (0, 0) if last else (second, blocks)
            jobs = [(at_ring(e), functools.partial(ring_event, e=e, last=last)) for e in range(half + 1)]
            if last:
                jobs += [(at_gather(e, half), functools.partial(gather_event, e=e)) for e in range(half + 1)]
            for lag, job in jobs:
                earliest, latest = base + tiles + lag, base + tiles * blocks + lag
                lo, hi = ((0, between), (between, second), (second, second + between), (second + between, 1 << 30))[phase]
                if latest < lo or earliest >= hi:
                    continue
                since = now - earliest
                if isinstance(now, int):
                    if since >= 0 and since % tiles == 0 and since // tiles < blocks:
                        job(first + since // tiles)
                else:

                    @pl.when((since >= 0) & (lax.rem(since + 64 * tiles, tiles) == 0) & (since < tiles * blocks))
                    def _(job=job, since=since, first=first):
                        job(first + lax.div(since, tiles))

    def forward(x_in, a0_out, a0t_out, h_out, wd0):
        def x_load(i, slot):
            return pltpu.make_async_copy(x_hbm.at[0, span(i, small)], x_in.at[slot], x_sem.at[slot])

        def stores(i, slot):
            return [
                pltpu.make_async_copy(a0_out.at[slot], a0_hbm.at[span(i, small)], in_sem.at[0, slot]),
                pltpu.make_async_copy(a0t_out.at[slot], a0t_hbm.at[:, span(i, small)], in_sem.at[1, slot]),
                pltpu.make_async_copy(h_out.at[slot], h_hbm.at[span(i, small)], dgu_sem.at[0, slot]),
            ]

        wd0_load = pltpu.make_async_copy(wd_hbm.at[0], wd0, wide_sem.at[2])
        x_load(0, 0).start()
        for copy in wide_loads(0):
            copy.start()
        wd0_load.start()
        for i in range(smalls):
            dy_load(i).start()
        for copy in weight_loads(0):
            copy.start()
        barrier = pltpu.get_barrier_semaphore()
        for k in range(1, n):
            pl.semaphore_signal(barrier, 1, device_id={"dp": lax.rem(me + k, n)}, device_id_type=MESH)
        squares[...] = jnp.zeros_like(squares)
        for copy in wide_loads(0):
            copy.wait()
        wd0_load.wait()

        @pl.loop(0, smalls)
        def _(i):
            slot = lax.rem(i, 2)
            x_load(i, slot).wait()

            @pl.when(i + 1 < smalls)
            def _():
                x_load(i + 1, 1 - slot).start()

            dy_load(i).wait()

            @pl.when(i >= 2)
            def _():
                for copy in stores(i - 2, slot):
                    copy.wait()

            gt[:, span(i, small)] = g[span(i, small)].T
            part = small // 2
            for c in range(2):
                here = pl.ds(c * part, part)
                rows = pl.ds(pl.multiple_of(i * small + c * part, part), part)
                x = x_in[slot, here]
                a0 = normed(x)
                a0_out[slot, here] = a0
                a0t_out[slot, :, here] = a0.T
                gate = dot(a0, wide[:, :ff])
                up = dot(a0, wide[:, ff:])
                z = (gate * jax.nn.sigmoid(gate) * up).astype(BF16)
                h = (x.astype(F32) + dot(z, wd0[...]).astype(BF16).astype(F32)).astype(BF16)
                h_out[slot, here] = h
                a1 = normed(h)
                a[rows] = a1
                at[:, rows] = a1.T
            for copy in stores(i, slot):
                copy.start()

        for i in range(max(smalls - 2, 0), smalls):
            for copy in stores(i, i % 2):
                copy.wait()
        pl.semaphore_wait(barrier, n - 1)

    def dgu_stores(b, t, slot):
        return [
            pltpu.make_async_copy(
                dgu.at[slot, :, pl.ds(i * block, block)],
                dgu_hbm.at[span(t, tile), pl.ds(pl.multiple_of(i * ff + b * block, block), block)],
                dgu_sem.at[i, slot],
            )
            for i in (0, 1)
        ]

    def steps(b, t, last):
        rows = span(t, tile)
        slot = lax.rem(b, 2)
        gu = dot(a[rows], wgu[slot])
        dz = dot(g[rows], wd[slot], BY_ROWS).astype(BF16).astype(F32)
        gate, up = gu[:, :block], gu[:, block:]
        s = jax.nn.sigmoid(gate)
        silu = gate * s
        z = (silu * up).astype(BF16)
        dgate = (dz * up * (s + silu * (1 - s))).astype(BF16)
        dup = (dz * silu).astype(BF16)
        both = jnp.concatenate([dgate, dup], 1)
        if last:
            dgu[lax.rem(t, 2)] = both
        acc_d[...] += dot(gt[:, rows], z)
        acc_gu[...] += dot(at[:, rows], both)

    def pack(b):
        slot = lax.rem(b, slots)
        of_d, of_block = d // n, block // n
        for s in range(n):
            for c in range(2 * block // LANES):
                piece = acc_gu[pl.ds(s * of_d, of_d), pl.ds(c * LANES, LANES)]
                own[slot, s, pl.ds(c * of_d, of_d)] = piece.astype(BF16)
        base = 2 * block // LANES * of_d
        for c in range(d // LANES):
            turned = acc_d[pl.ds(c * LANES, LANES)].T.astype(BF16)
            for s in range(n):
                own[slot, s, pl.ds(base + c * of_block, of_block)] = turned[s * of_block : (s + 1) * of_block]

    def one_block(b, last):
        @pl.when(b + 1 < units)
        def _():
            for copy in weight_loads(b + 1):
                copy.start()

        for copy in weight_loads(b):
            copy.wait()
        acc_gu[...] = jnp.zeros_like(acc_gu)
        acc_d[...] = jnp.zeros_like(acc_d)

        @pl.loop(0, tiles)
        def _(t):
            if last:

                @pl.when((b > 0) | (t > 1))
                def _():
                    for copy in dgu_stores(b, t, lax.rem(t, 2)):
                        copy.wait()

            else:

                @pl.when(b == blocks)
                def _():
                    for copy in a0_loads(t):
                        copy.wait()

            steps(b, t, last)
            if last:
                for copy in dgu_stores(b, t, lax.rem(t, 2)):
                    copy.start()
                events(b * tiles + t, 0)
            else:
                events(second + (b - blocks) * tiles + t, 2)

        pack(b)

    def way_back(d_in, h_in):
        def in_loads(i, slot):
            return [
                pltpu.make_async_copy(dgu_hbm.at[span(i, small)], d_in.at[slot], dy_sem.at[slot]),
                pltpu.make_async_copy(h_hbm.at[span(i, small)], h_in.at[slot], dy_sem.at[2 + slot]),
            ]

        for copy in in_loads(0, 0):
            copy.start()
        for t in range(tiles):
            for copy in a0_loads(t):
                copy.start()
        for copy in wide_loads(1):
            copy.wait()

        @pl.loop(0, smalls)
        def _(i):
            slot = lax.rem(i, 2)
            for copy in in_loads(i, slot):
                copy.wait()

            @pl.when(i + 1 < smalls)
            def _():
                for copy in in_loads(i + 1, 1 - slot):
                    copy.start()

            part = small // 2
            for c in range(2):
                here = pl.ds(c * part, part)
                rows = pl.ds(pl.multiple_of(i * small + c * part, part), part)
                by_a = dot(d_in[slot, here], wide[...], BY_ROWS).astype(BF16).astype(F32)
                h = h_in[slot, here].astype(F32)
                scale = scale_of(h)
                along = jnp.mean(by_a * h, -1, keepdims=True)
                by_h = (by_a * scale - h * (scale * scale * scale * along)).astype(BF16)
                out = (g[rows].astype(F32) + by_h.astype(F32)).astype(BF16)
                g[rows] = out
                gt[:, rows] = out.T
            events(between + i, 1)

    pl.run_scoped(
        forward,
        pltpu.VMEM((2, small, d), BF16),
        pltpu.VMEM((2, small, d), BF16),
        pltpu.VMEM((2, d, small), BF16),
        pltpu.VMEM((2, small, d), BF16),
        pltpu.VMEM((ff, d), BF16),
    )
    for copy in wide_loads(1):
        copy.start()

    @pl.loop(0, blocks)
    def _(b):
        one_block(b, True)

    for t in (tiles - 2, tiles - 1):
        for copy in dgu_stores(blocks - 1, t, t % 2):
            copy.wait()
    pl.run_scoped(way_back, pltpu.VMEM((2, small, 2 * ff), BF16), pltpu.VMEM((2, small, d), BF16))

    @pl.loop(blocks, units)
    def _(b):
        one_block(b, False)

    for now in range(second + between, second + between + at_ring(half) + 1):
        events(now, 3)

    def part_copy(k):
        return pltpu.make_async_remote_copy(
            src_ref=squares,
            dst_ref=parts.at[me],
            send_sem=part_send.at[k - 1],
            recv_sem=part_recv.at[k - 1],
            device_id={"dp": lax.rem(me + k, n)},
            device_id_type=MESH,
        )

    for k in range(1, n):
        part_copy(k).start()
    parts[me] = squares[...]
    for k in range(1, n):
        part_copy(k).wait()
    total = parts[0]
    for k in range(1, n):
        total = total + parts[k]
    total_ref[...] = total


def reduced(n, x, dy, w_gate, w_up, w_down):
    tokens, d = x.shape[1:]
    ff = w_gate.shape[2]
    block, tile = BLOCK, tokens // 4
    tiles, blocks, half = tokens // tile, ff // block, n // 2
    small, smalls = tile // 2, 2 * tiles
    shard_rows = 3 * d * block // (n * LANES)
    slots = at_ring(half) // tiles + 2
    anywhere, vmem = pl.BlockSpec(memory_space=pl.ANY), pl.BlockSpec(memory_space=pltpu.VMEM)
    dma = pltpu.SemaphoreType.DMA
    return pl.pallas_call(
        functools.partial(main_kernel, n),
        in_specs=[anywhere] * 5,
        out_specs=[anywhere, vmem, vmem, vmem] + [anywhere] * 4,
        out_shape=[
            jax.ShapeDtypeStruct((n, blocks, shard_rows, LANES), BF16),
            jax.ShapeDtypeStruct((blocks // 2, shard_rows, LANES), BF16),
            jax.ShapeDtypeStruct((blocks // 2, shard_rows, LANES), BF16),
            jax.ShapeDtypeStruct((8, LANES), F32),
            jax.ShapeDtypeStruct((tokens, d), BF16),
            jax.ShapeDtypeStruct((d, tokens), BF16),
            jax.ShapeDtypeStruct((tokens, d), BF16),
            jax.ShapeDtypeStruct((tokens, 2 * ff), BF16),
        ],
        scratch_shapes=[
            pltpu.VMEM((tokens, d), BF16),
            pltpu.VMEM((d, tokens), BF16),
            pltpu.VMEM((tokens, d), BF16),
            pltpu.VMEM((d, tokens), BF16),
            pltpu.VMEM((d, 2 * ff), BF16),
            pltpu.VMEM((2, d, 2 * block), BF16),
            pltpu.VMEM((2, block, d), BF16),
            pltpu.VMEM((d, 2 * block), F32),
            pltpu.VMEM((d, block), F32),
            pltpu.VMEM((2, tile, 2 * block), BF16),
            pltpu.VMEM((slots, n, shard_rows, LANES), BF16),
            pltpu.VMEM((slots, half, shard_rows, LANES), BF16),
            pltpu.VMEM((slots, half, shard_rows, LANES), BF16),
            pltpu.VMEM((blocks, shard_rows, LANES), BF16),
            pltpu.VMEM((8, LANES), F32),
            pltpu.VMEM((n, 8, LANES), F32),
            dma((2,)),
            dma((smalls,)),
            dma((3,)),
            dma((3, 2)),
            dma((2, 2)),
            dma((2, tiles)),
            dma((2, slots, half)),
            dma((2, slots, half)),
            dma((2, blocks, half)),
            dma((2, blocks, half)),
            dma((blocks,)),
            dma((n - 1,)),
            dma((n - 1,)),
            pltpu.SemaphoreType.REGULAR((2,)),
        ],
        compiler_params=pltpu.CompilerParams(collective_id=0, has_side_effects=True, vmem_limit_bytes=67_043_328),
        cost_estimate=pl.CostEstimate(flops=34 * tokens * d * ff, bytes_accessed=16 * tokens * d, transcendentals=3 * tokens * ff),
        name="reduced",
    )(x, dy, w_gate, w_up, w_down)[:4]


def update_kernel(count, n_terms, n_aliased, shards, total_ref, *refs):
    terms, refs = refs[:n_terms], refs[n_terms:]
    w, m, v = refs[:3], refs[3:6], refs[6:9]
    new_w, new_m, new_v = (refs[9 + n_aliased + 3 * i : 12 + n_aliased + 3 * i] for i in range(3))
    factor = jnp.minimum(1.0, 0.5 * lax.rsqrt(jnp.sum(total_ref[...], keepdims=True) / count + 1e-30))
    units = terms[0].shape[0]
    of_d, block = w[0].shape[0], w[0].shape[1] // units
    of_block, d = w[2].shape[1:]
    slabs = block // LANES

    def one(i, where, term):
        term = term.astype(F32) * factor
        m_new = 0.9 * m[i][where] + 0.1 * term
        v_new = 0.95 * v[i][where] + 0.05 * term * term
        wide = w[i][where].astype(F32)
        new_m[i][where] = m_new
        new_v[i][where] = v_new
        new_w[i][where] = (wide - 0.02 * (m_new * lax.rsqrt(v_new + 1e-8) + 0.1 * wide)).astype(BF16)

    def apply(term):
        for j in range(units):
            for i in range(2):
                for c in range(slabs):
                    one(i, (slice(None), pl.ds(j * block + c * LANES, LANES)), term[j, pl.ds((i * slabs + c) * of_d, of_d)])
            for c in range(d // LANES):
                one(2, (j, slice(None), pl.ds(c * LANES, LANES)), term[j, pl.ds(2 * slabs * of_d + c * of_block, of_block)])

    if n_terms == 1:
        apply(terms[0])
    else:
        for k, term in enumerate(terms):

            @pl.when(pl.program_id(0) * 2 + pl.program_id(1) == k)
            def _(term=term):
                apply(term)


def update(layer, shards, terms, total, weights, m, v, so_far):
    _, d, ff = weights[0].shape
    _, blocks, n, of_block, _ = weights[2].shape
    of_d = d // n
    flat = pl.BlockSpec((None, of_d, ff // 2), lambda i, c, shards: (layer, shards[i], c))
    tall = pl.BlockSpec((None, blocks // 2, None, of_block, d), lambda i, c, shards: (layer, c, shards[i], 0, 0))
    if isinstance(terms, tuple):
        array, first = terms
        terms = [array]
        term = pl.BlockSpec((None, blocks // 2, *array.shape[2:]), lambda i, c, shards: (first + i, c, 0, 0))
    else:
        term = pl.BlockSpec(terms[0].shape, lambda i, c, shards: (0, 0, 0))
    arrays = [*weights, *m, *v]
    specs = [flat, flat, tall] * 3
    aliased = list(so_far) if so_far is not None else []
    start = 2 + len(terms) + len(arrays)
    n_shards = shards.shape[0]
    bytes_accessed = n_shards * 22 * 3 * d * ff // n
    return pl.pallas_call(
        functools.partial(update_kernel, 3 * weights[0].size, len(terms), len(aliased)),
        grid_spec=pltpu.PrefetchScalarGridSpec(
            num_scalar_prefetch=1,
            grid=(n_shards, 2),
            in_specs=[pl.BlockSpec((8, LANES), lambda i, c, shards: (0, 0))]
            + [term] * len(terms)
            + specs
            + [pl.BlockSpec(memory_space=pl.ANY)] * len(aliased),
            out_specs=specs,
        ),
        out_shape=[jax.ShapeDtypeStruct(one.shape, one.dtype) for one in arrays],
        input_output_aliases={start + i: i for i in range(len(aliased))},
        compiler_params=pltpu.CompilerParams(vmem_limit_bytes=63 << 20),
        cost_estimate=pl.CostEstimate(flops=300 * bytes_accessed, bytes_accessed=bytes_accessed, transcendentals=0),
        name=f"update_{layer}",
    )(shards, total, *terms, *arrays, *aliased)


def solution(mesh):
    n = mesh.shape["dp"]
    half = n // 2

    def step(x, dy, *arrays):
        weights, m, v = (list(arrays[i : i + 3]) for i in (0, 3, 6))
        g1, g0a, g0b, total = reduced(n, x, dy, *weights)

        layers, ff, d = weights[2].shape
        split = (layers, ff // BLOCK, n, BLOCK // n, d)
        for group in (weights, m, v):
            group[2] = group[2].reshape(split)
        back = lax.rem(lax.axis_index("dp") + n - jnp.arange(n, dtype=jnp.int32), n)

        def sent(value, by):
            return lax.ppermute(value, "dp", [(i, (i + by) % n) for i in range(n)])

        came = [(g0a, g0b)]
        right, left = (g0a, g0b), (g0a, g0b)
        for k in range(1, half):
            a = sent(right[0], 1), sent(left[0], -1)
            b = sent(right[1], 1), sent(left[1], -1)
            right, left = (a[0], b[0]), (a[1], b[1])
            came.append((*right, *left))
        came.append((sent(right[0], 1), sent(left[1], -1)))

        def after(places, *values):
            return lax.optimization_barrier((places, *values))[0]

        out = update(1, back[:half], (g1, 0), total, weights, m, v, None)
        out = update(1, after(back[half:], *came[1][0::2]), (g1, half), total, weights, m, v, out)
        for k in range(half + 1):
            places = jnp.stack([back[k]] if k in (0, half) else [back[k], back[n - k]])
            if k == 0:
                places = after(places, *came[1][1::2])
            elif k == 1:
                places = after(places, *came[2][0::2])
            out = update(0, places, list(came[k]), total, weights, m, v, out)
        out = list(out)
        for i in (2, 5, 8):
            out[i] = out[i].reshape(layers, ff, d)
        return tuple(out)

    return jax.shard_map(
        step,
        mesh=mesh,
        in_specs=(P(("rep", "dp"), None, None),) * 2 + (P(None, None, None),) * 9,
        out_specs=(P("rep", None, None),) * 9,
        check_vma=False,
    )
```

```python
import functools

import jax
import jax.numpy as jnp
from jax import lax
from jax.experimental import pallas as pl
from jax.experimental.pallas import tpu as pltpu
from jax.sharding import PartitionSpec as P


BF16, F32 = jnp.bfloat16, jnp.float32
MESH = pl.DeviceIdType.MESH
LANES = 128
BLOCK = 256
PLAIN, BY_ROWS = ((1,), (0,)), ((1,), (1,))


def dot(a, b, contract=PLAIN):
    return lax.dot_general(a, b, (contract, ((), ())), preferred_element_type=F32)


def scale_of(wide):
    return lax.rsqrt(jnp.mean(wide * wide, -1, keepdims=True) + 1e-6)


def normed(h):
    wide = h.astype(F32)
    return (wide * scale_of(wide)).astype(BF16)


def when(condition, do):
    if isinstance(condition, bool):
        if condition:
            do()
    else:
        pl.when(condition)(do)


def at_ring(e):
    return 5 * e // 2


def at_gather(e, half):
    return at_ring(half) + 3 * e


def main_kernel(
    n, x_hbm, dy_hbm, wg_hbm, wu_hbm, wd_hbm,
    g1_hbm, g0a_ref, g0b_ref, total_ref, a0t_hbm, h_hbm, dgu_hbm, gu_hbm,
    a, at, g, gt, wide, wgu, wd, acc_gu, acc_d, dgu, own, from_left, from_right, kept, squares, parts,
    x_sem, dy_sem, wide_sem, w_sem, dgu_sem, in_sem, send_sem, recv_sem, there_sem, here_sem, kept_sem, part_send, part_recv, credit,
):
    tokens, d = a.shape
    ff = wg_hbm.shape[2]
    block = wd.shape[1]
    blocks = ff // block
    units, half = 2 * blocks, n // 2
    tile = dgu.shape[1]
    tiles = tokens // tile
    small = tile // 2
    smalls = tokens // small
    chunk = small // 2
    chunks = tokens // chunk
    slots, shard_rows = own.shape[0], own.shape[2]
    me = lax.axis_index("dp")
    right, left = lax.rem(me + 1, n), lax.rem(me + n - 1, n)

    def span(i, size):
        return pl.ds(i * size, size) if isinstance(i, int) else pl.ds(pl.multiple_of(i * size, size), size)

    def dy_load(i):
        return pltpu.make_async_copy(dy_hbm.at[0, span(i, chunk)], g.at[span(i, chunk)], dy_sem.at[i])

    def wide_loads(layer):
        return [
            pltpu.make_async_copy(wg_hbm.at[layer], wide.at[:, pl.ds(0, ff)], wide_sem.at[0]),
            pltpu.make_async_copy(wu_hbm.at[layer], wide.at[:, pl.ds(ff, ff)], wide_sem.at[1]),
        ]

    def a0t_load(t):
        return pltpu.make_async_copy(a0t_hbm.at[:, span(t, tile)], at.at[:, span(t, tile)], in_sem.at[t])

    def gu_loads(b):
        slot = lax.rem(b, 2)
        return [
            pltpu.make_async_copy(ref.at[1, :, span(b, block)], wgu.at[slot, :, pl.ds(i * block, block)], w_sem.at[i, slot])
            for i, ref in enumerate((wg_hbm, wu_hbm))
        ]

    def down_load(b):
        last = jnp.int32(b < blocks) if isinstance(b, int) else (b < blocks).astype(jnp.int32)
        slot = lax.rem(b, 2)
        return pltpu.make_async_copy(wd_hbm.at[last, span(b - blocks * (1 - last), block), :], wd.at[slot], w_sem.at[2, slot])

    def ring_copy(u, k, way):
        slot = lax.rem(u, slots)
        ahead = half - k if way == 0 else n - half + k
        shard = lax.rem(me + ahead, n)
        rows = pl.ds(0, shard_rows)
        if k == 0:
            rows = pl.ds(way * (shard_rows // 2), shard_rows // 2)
        return pltpu.make_async_remote_copy(
            src_ref=own.at[slot, shard, rows],
            dst_ref=(from_left, from_right)[way].at[slot, k, rows],
            send_sem=send_sem.at[way, slot, k],
            recv_sem=recv_sem.at[way, slot, k],
            device_id={"dp": (right, left)[way]},
            device_id_type=MESH,
        )

    def ring_event(u, e, last):
        slot = lax.rem(u, slots)
        if e == 0:

            def take():
                pl.semaphore_wait(credit.at[0], 1)
                pl.semaphore_wait(credit.at[1], 1)

            when(u >= slots, take)
        else:
            for way in (0, 1):
                ring_copy(u, e - 1, way).wait()
        if 0 < e < half:
            for way in (0, 1):
                shard = lax.rem(me + (half - e if way == 0 else n - half + e), n)
                rows = pl.ds(0, shard_rows) if e > 1 else pl.ds(way * (shard_rows // 2), shard_rows // 2)
                came = (from_left, from_right)[way][slot, e - 1, rows].astype(F32)
                own[slot, shard, rows] = (own[slot, shard, rows].astype(F32) + came).astype(BF16)
        if e < half:
            for way in (0, 1):
                ring_copy(u, e, way).start()
        else:
            came = from_left[slot, e - 1].astype(F32) + from_right[slot, e - 1].astype(F32)
            done = (own[slot, me].astype(F32) + came).astype(BF16)
            if last:
                kept[u] = done
            else:

                def keep(ref, place):
                    def do():
                        ref[place] = done

                    return do

                cut = blocks + blocks // 2
                when(u < cut, keep(g0a_ref, jnp.minimum(u - blocks, blocks // 2 - 1)))
                when(u >= cut, keep(g0b_ref, jnp.maximum(u - cut, 0)))
            exact = done.astype(F32)
            squares[...] += jnp.sum((exact * exact).reshape(shard_rows // 8, 8, LANES), 0)

            def give():
                pl.semaphore_signal(credit.at[0], 1, device_id={"dp": left}, device_id_type=MESH)
                pl.semaphore_signal(credit.at[1], 1, device_id={"dp": right}, device_id_type=MESH)

            when(u < units - slots, give)

    def gather_copy(u, k, way):
        rows = pl.ds(0, shard_rows)
        if k == half - 1:
            rows = pl.ds(way * (shard_rows // 2), shard_rows // 2)
        place = (k, n - k)[way]
        after = (k + 1, n - k - 1)[way]
        return pltpu.make_async_remote_copy(
            src_ref=kept.at[u, rows] if k == 0 else g1_hbm.at[place, u, rows],
            dst_ref=g1_hbm.at[after, u, rows],
            send_sem=there_sem.at[way, u, k],
            recv_sem=here_sem.at[way, u, k],
            device_id={"dp": (right, left)[way]},
            device_id_type=MESH,
        )

    def kept_copy(u):
        return pltpu.make_async_copy(kept.at[u], g1_hbm.at[0, u], kept_sem.at[u])

    def gather_event(u, e):
        if e == 0:
            kept_copy(u).start()
        else:
            for way in (0, 1):
                gather_copy(u, e - 1, way).wait()
        if e < half:
            for way in (0, 1):
                gather_copy(u, e, way).start()
        else:
            kept_copy(u).wait()

    between = tiles * blocks
    second = between + smalls

    def events(now, phase):
        for last in (True, False):
            base, first = (0, 0) if last else (second, blocks)
            jobs = [(at_ring(e), functools.partial(ring_event, e=e, last=last)) for e in range(half + 1)]
            if last:
                jobs += [(at_gather(e, half), functools.partial(gather_event, e=e)) for e in range(half + 1)]
            for lag, job in jobs:
                earliest, latest = base + tiles + lag, base + tiles * blocks + lag
                lo, hi = ((0, between), (between, second), (second, second + between), (second + between, 1 << 30))[phase]
                if latest < lo or earliest >= hi:
                    continue
                since = now - earliest
                if isinstance(now, int):
                    if since >= 0 and since % tiles == 0 and since // tiles < blocks:
                        job(first + since // tiles)
                else:

                    @pl.when((since >= 0) & (lax.rem(since + 64 * tiles, tiles) == 0) & (since < tiles * blocks))
                    def _(job=job, since=since, first=first):
                        job(first + lax.div(since, tiles))

    def forward(x_in, a0t_out, h_out, z, gu_out, wd0):
        def x_load(i):
            slot = lax.rem(i, 4)
            return pltpu.make_async_copy(x_hbm.at[0, span(i, chunk)], x_in.at[slot], x_sem.at[slot])

        def first_stores(i):
            slot = lax.rem(i, 2)
            return [
                pltpu.make_async_copy(a0t_out.at[slot], a0t_hbm.at[:, span(i, chunk)], in_sem.at[slot]),
                pltpu.make_async_copy(gu_out.at[slot], gu_hbm.at[span(i, chunk)], dgu_sem.at[0, slot]),
            ]

        def second_store(i):
            slot = lax.rem(i, 2)
            return pltpu.make_async_copy(h_out.at[slot], h_hbm.at[span(i, chunk)], dgu_sem.at[1, slot])

        def first(i):
            slot = lax.rem(i, 2)
            a0 = normed(x_in[lax.rem(i, 4)])
            a0t_out[slot] = a0.T
            cut = 2 * block
            for c in range(ff // cut):
                gate = dot(a0, wide[:, c * cut : (c + 1) * cut])
                up = dot(a0, wide[:, ff + c * cut : ff + (c + 1) * cut])
                gu_out[slot, :, pl.ds(c * cut, cut)] = gate
                gu_out[slot, :, pl.ds(ff + c * cut, cut)] = up
                z[slot, :, pl.ds(c * cut, cut)] = (gate * jax.nn.sigmoid(gate) * up).astype(BF16)

        def second(i):
            slot = lax.rem(i, 2)
            rows = span(i, chunk)
            h = (x_in[lax.rem(i, 4)].astype(F32) + dot(z[slot], wd0[...]).astype(BF16).astype(F32)).astype(BF16)
            h_out[slot] = h
            a1 = normed(h)
            a[rows] = a1
            at[:, rows] = a1.T
            gt[:, rows] = g[rows].T

        wd0_load = pltpu.make_async_copy(wd_hbm.at[0], wd0, wide_sem.at[2])
        x_load(0).start()
        for copy in wide_loads(0):
            copy.start()
        wd0_load.start()
        for i in (1, 2):
            x_load(i).start()
        for i in range(chunks):
            dy_load(i).start()
        for copy in gu_loads(0):
            copy.start()
        down_load(0).start()
        barrier = pltpu.get_barrier_semaphore()
        for k in range(1, n):
            pl.semaphore_signal(barrier, 1, device_id={"dp": lax.rem(me + k, n)}, device_id_type=MESH)
        squares[...] = jnp.zeros_like(squares)
        x_load(0).wait()
        for copy in wide_loads(0):
            copy.wait()
        first(0)
        for copy in first_stores(0):
            copy.start()
        wd0_load.wait()

        @pl.loop(1, chunks)
        def _(i):
            x_load(i).wait()
            dy_load(i - 1).wait()

            @pl.when(i >= 2)
            def _():
                for copy in first_stores(i - 2):
                    copy.wait()

            @pl.when(i >= 3)
            def _():
                second_store(i - 3).wait()

            second(i - 1)
            first(i)
            for copy in first_stores(i):
                copy.start()
            second_store(i - 1).start()

            @pl.when(i + 2 < chunks)
            def _():
                x_load(i + 2).start()

        dy_load(chunks - 1).wait()
        second_store(chunks - 3).wait()
        second(chunks - 1)
        second_store(chunks - 1).start()
        for i in (chunks - 2, chunks - 1):
            for copy in first_stores(i):
                copy.wait()
            second_store(i).wait()
        pl.semaphore_wait(barrier, n - 1)

    def dgu_stores(b, t, slot):
        return [
            pltpu.make_async_copy(
                dgu.at[slot, :, pl.ds(i * block, block)],
                dgu_hbm.at[span(t, tile), pl.ds(pl.multiple_of(i * ff + b * block, block), block)],
                dgu_sem.at[i, slot],
            )
            for i in (0, 1)
        ]

    def steps(b, t, gu_in):
        rows = span(t, tile)
        slot = lax.rem(b, 2)
        gu = gu_in[lax.rem(t, 2)] if gu_in is not None else dot(a[rows], wgu[slot])
        dz = dot(g[rows], wd[slot], BY_ROWS).astype(BF16).astype(F32)
        gate, up = gu[:, :block], gu[:, block:]
        s = jax.nn.sigmoid(gate)
        silu = gate * s
        z = (silu * up).astype(BF16)
        dgate = (dz * up * (s + silu * (1 - s))).astype(BF16)
        dup = (dz * silu).astype(BF16)
        both = jnp.concatenate([dgate, dup], 1)
        if gu_in is None:
            dgu[lax.rem(t, 2)] = both
        acc_d[...] += dot(gt[:, rows], z)
        acc_gu[...] += dot(at[:, rows], both)

    def pack(b):
        slot = lax.rem(b, slots)
        of_d, of_block = d // n, block // n
        for s in range(n):
            for c in range(2 * block // LANES):
                piece = acc_gu[pl.ds(s * of_d, of_d), pl.ds(c * LANES, LANES)]
                own[slot, s, pl.ds(c * of_d, of_d)] = piece.astype(BF16)
        base = 2 * block // LANES * of_d
        for c in range(d // LANES):
            turned = acc_d[pl.ds(c * LANES, LANES)].T.astype(BF16)
            for s in range(n):
                own[slot, s, pl.ds(base + c * of_block, of_block)] = turned[s * of_block : (s + 1) * of_block]

    def clear():
        acc_gu[...] = jnp.zeros_like(acc_gu)
        acc_d[...] = jnp.zeros_like(acc_d)

    def last_block(b):
        @pl.when(b + 1 < blocks)
        def _():
            for copy in gu_loads(b + 1):
                copy.start()

        down_load(b + 1).start()
        for copy in gu_loads(b):
            copy.wait()
        down_load(b).wait()
        clear()

        @pl.loop(0, tiles)
        def _(t):
            @pl.when((b > 0) | (t > 1))
            def _():
                for copy in dgu_stores(b, t, lax.rem(t, 2)):
                    copy.wait()

            steps(b, t, None)
            for copy in dgu_stores(b, t, lax.rem(t, 2)):
                copy.start()
            events(b * tiles + t, 0)

        pack(b)

    def first_blocks(gu_in):
        def tile_loads(b, t):
            slot = lax.rem(t, 2)
            return [
                pltpu.make_async_copy(
                    gu_hbm.at[span(t, tile), pl.ds(pl.multiple_of(i * ff + (b - blocks) * block, block), block)],
                    gu_in.at[slot, :, pl.ds(i * block, block)],
                    dgu_sem.at[i, slot],
                )
                for i in (0, 1)
            ]

        for copy in tile_loads(blocks, 0):
            copy.start()

        @pl.loop(blocks, units)
        def _(b):
            @pl.when(b + 1 < units)
            def _():
                down_load(b + 1).start()

            down_load(b).wait()
            clear()

            @pl.loop(0, tiles)
            def _(t):
                @pl.when(b == blocks)
                def _():
                    a0t_load(t).wait()

                for copy in tile_loads(b, t):
                    copy.wait()
                ends = t == tiles - 1

                @pl.when((b + 1 < units) | jnp.logical_not(ends))
                def _():
                    for copy in tile_loads(jnp.where(ends, b + 1, b), jnp.where(ends, 0, t + 1)):
                        copy.start()

                steps(b, t, gu_in)
                events(second + (b - blocks) * tiles + t, 2)

            pack(b)

    def way_back(d_in, h_in):
        def in_loads(i, slot):
            return [
                pltpu.make_async_copy(dgu_hbm.at[span(i, small)], d_in.at[slot], dy_sem.at[slot]),
                pltpu.make_async_copy(h_hbm.at[span(i, small)], h_in.at[slot], dy_sem.at[2 + slot]),
            ]

        for copy in in_loads(0, 0):
            copy.start()
        for t in range(tiles):
            a0t_load(t).start()
        for copy in wide_loads(1):
            copy.wait()

        @pl.loop(0, smalls)
        def _(i):
            slot = lax.rem(i, 2)
            for copy in in_loads(i, slot):
                copy.wait()

            @pl.when(i + 1 < smalls)
            def _():
                for copy in in_loads(i + 1, 1 - slot):
                    copy.start()

            part = small // 2
            for c in range(2):
                here = pl.ds(c * part, part)
                rows = pl.ds(pl.multiple_of(i * small + c * part, part), part)
                by_a = dot(d_in[slot, here], wide[...], BY_ROWS).astype(BF16).astype(F32)
                h = h_in[slot, here].astype(F32)
                scale = scale_of(h)
                along = jnp.mean(by_a * h, -1, keepdims=True)
                by_h = (by_a * scale - h * (scale * scale * scale * along)).astype(BF16)
                out = (g[rows].astype(F32) + by_h.astype(F32)).astype(BF16)
                g[rows] = out
                gt[:, rows] = out.T
            events(between + i, 1)

    pl.run_scoped(
        forward,
        pltpu.VMEM((4, chunk, d), BF16),
        pltpu.VMEM((2, d, chunk), BF16),
        pltpu.VMEM((2, chunk, d), BF16),
        pltpu.VMEM((2, chunk, ff), BF16),
        pltpu.VMEM((2, chunk, 2 * ff), F32),
        pltpu.VMEM((ff, d), BF16),
    )
    for copy in wide_loads(1):
        copy.start()

    @pl.loop(0, blocks)
    def _(b):
        last_block(b)

    for t in (tiles - 2, tiles - 1):
        for copy in dgu_stores(blocks - 1, t, t % 2):
            copy.wait()
    pl.run_scoped(way_back, pltpu.VMEM((2, small, 2 * ff), BF16), pltpu.VMEM((2, small, d), BF16))
    pl.run_scoped(first_blocks, pltpu.VMEM((2, tile, 2 * block), F32))
    for now in range(second + between, second + between + at_ring(half) + 1):
        events(now, 3)

    def part_copy(k):
        return pltpu.make_async_remote_copy(
            src_ref=squares,
            dst_ref=parts.at[me],
            send_sem=part_send.at[k - 1],
            recv_sem=part_recv.at[k - 1],
            device_id={"dp": lax.rem(me + k, n)},
            device_id_type=MESH,
        )

    for k in range(1, n):
        part_copy(k).start()
    parts[me] = squares[...]
    for k in range(1, n):
        part_copy(k).wait()
    total = parts[0]
    for k in range(1, n):
        total = total + parts[k]
    total_ref[...] = total


def reduced(n, x, dy, w_gate, w_up, w_down):
    tokens, d = x.shape[1:]
    ff = w_gate.shape[2]
    block, tile = BLOCK, tokens // 4
    tiles, blocks, half = tokens // tile, ff // block, n // 2
    smalls = 2 * tiles
    shard_rows = 3 * d * block // (n * LANES)
    slots = at_ring(half) // tiles + 2
    anywhere, vmem = pl.BlockSpec(memory_space=pl.ANY), pl.BlockSpec(memory_space=pltpu.VMEM)
    dma = pltpu.SemaphoreType.DMA
    return pl.pallas_call(
        functools.partial(main_kernel, n),
        in_specs=[anywhere] * 5,
        out_specs=[anywhere, vmem, vmem, vmem] + [anywhere] * 4,
        out_shape=[
            jax.ShapeDtypeStruct((n, blocks, shard_rows, LANES), BF16),
            jax.ShapeDtypeStruct((blocks // 2, shard_rows, LANES), BF16),
            jax.ShapeDtypeStruct((blocks // 2, shard_rows, LANES), BF16),
            jax.ShapeDtypeStruct((8, LANES), F32),
            jax.ShapeDtypeStruct((d, tokens), BF16),
            jax.ShapeDtypeStruct((tokens, d), BF16),
            jax.ShapeDtypeStruct((tokens, 2 * ff), BF16),
            jax.ShapeDtypeStruct((tokens, 2 * ff), F32),
        ],
        scratch_shapes=[
            pltpu.VMEM((tokens, d), BF16),
            pltpu.VMEM((d, tokens), BF16),
            pltpu.VMEM((tokens, d), BF16),
            pltpu.VMEM((d, tokens), BF16),
            pltpu.VMEM((d, 2 * ff), BF16),
            pltpu.VMEM((2, d, 2 * block), BF16),
            pltpu.VMEM((2, block, d), BF16),
            pltpu.VMEM((d, 2 * block), F32),
            pltpu.VMEM((d, block), F32),
            pltpu.VMEM((2, tile, 2 * block), BF16),
            pltpu.VMEM((slots, n, shard_rows, LANES), BF16),
            pltpu.VMEM((slots, half, shard_rows, LANES), BF16),
            pltpu.VMEM((slots, half, shard_rows, LANES), BF16),
            pltpu.VMEM((blocks, shard_rows, LANES), BF16),
            pltpu.VMEM((8, LANES), F32),
            pltpu.VMEM((n, 8, LANES), F32),
            dma((4,)),
            dma((2 * smalls,)),
            dma((3,)),
            dma((3, 2)),
            dma((2, 2)),
            dma((tiles,)),
            dma((2, slots, half)),
            dma((2, slots, half)),
            dma((2, blocks, half)),
            dma((2, blocks, half)),
            dma((blocks,)),
            dma((n - 1,)),
            dma((n - 1,)),
            pltpu.SemaphoreType.REGULAR((2,)),
        ],
        compiler_params=pltpu.CompilerParams(collective_id=0, has_side_effects=True, vmem_limit_bytes=67_043_328),
        cost_estimate=pl.CostEstimate(flops=34 * tokens * d * ff, bytes_accessed=16 * tokens * d, transcendentals=3 * tokens * ff),
        name="reduced",
    )(x, dy, w_gate, w_up, w_down)[:4]


def update_kernel(n, layer, places, count, n_terms, *refs):
    n_items = 2 * len(places)
    total_ref, terms, (w, m, v) = refs[0], refs[1 : 1 + n_terms], (refs[1 + n_terms + 3 * i : 4 + n_terms + 3 * i] for i in range(3))
    *refs, flat_w, tall_w, flat, tall, grads, in_sem, out_sem = refs[10 + n_terms :]
    new = [refs[len(refs) - 9 + 3 * i : len(refs) - 6 + 3 * i] for i in range(3)]
    _, units, _, _ = grads.shape
    _, _, of_d, width = flat_w.shape
    of_block, d = tall_w.shape[2:]
    block = width // units
    slabs = block // LANES
    me = lax.axis_index("dp")

    def place(k):
        if isinstance(k, int):
            return places[k // 2]
        found = jnp.int32(places[0])
        for i, at in enumerate(places):
            found = jnp.where(lax.div(k, 2) == i, at, found)
        return found

    def copies(k, arrays, back):
        shard = lax.rem(me + n - place(k), n)
        half = lax.rem(k, 2)
        across = pl.ds(pl.multiple_of(shard * of_d, of_d), of_d), pl.ds(pl.multiple_of(half * width, width), width)
        pairs = []
        for kind, (first, second, third) in enumerate(arrays):
            for i, ref in enumerate((first, second)):
                pairs.append((ref.at[layer, *across], flat_w.at[k, i] if kind == 0 else flat.at[k, kind - 1, i]))
            pairs.append((third.at[layer, pl.ds(half * units, units), shard], tall_w.at[k] if kind == 0 else tall.at[k, kind - 1]))
        sem = out_sem.at[k] if back else in_sem.at[k]
        return [pltpu.make_async_copy(*(pair[::-1] if back else pair), sem) for pair in pairs]

    def term_copy(k):
        if n_terms == 1:
            ref = terms[0].at[place(k), pl.ds(k % 2 * units, units)]
        else:
            ref = terms[k]
        return pltpu.make_async_copy(ref, grads.at[k], in_sem.at[k])

    for k in range(n_items):
        for copy in [term_copy(k), *copies(k, (w, m, v), False)]:
            copy.start()
    factor = jnp.minimum(1.0, 0.5 * lax.rsqrt(jnp.sum(total_ref[...], keepdims=True) / count + 1e-30))

    @pl.loop(0, n_items)
    def _(k):
        pltpu.make_async_copy(grads.at[k], grads.at[k], in_sem.at[k]).wait()
        for copy in copies(k, (w, m, v), False):
            copy.wait()

        def one(w_ref, m_ref, v_ref, where, term):
            term = term.astype(F32) * factor
            m_new = 0.9 * m_ref[where] + 0.1 * term
            v_new = 0.95 * v_ref[where] + 0.05 * term * term
            wide = w_ref[where].astype(F32)
            m_ref[where] = m_new
            v_ref[where] = v_new
            w_ref[where] = (wide - 0.02 * (m_new * lax.rsqrt(v_new + 1e-8) + 0.1 * wide)).astype(BF16)

        for j in range(units):
            for i in range(2):
                for c in range(slabs):
                    where = slice(None), pl.ds(j * block + c * LANES, LANES)
                    term = grads[k, j, pl.ds((i * slabs + c) * of_d, of_d)]
                    one(flat_w.at[k, i], flat.at[k, 0, i], flat.at[k, 1, i], where, term)
            for c in range(d // LANES):
                where = j, slice(None), pl.ds(c * LANES, LANES)
                term = grads[k, j, pl.ds(2 * slabs * of_d + c * of_block, of_block)]
                one(tall_w.at[k], tall.at[k, 0], tall.at[k, 1], where, term)
        for copy in copies(k, new, True):
            copy.start()

    @pl.loop(0, n_items)
    def _(k):
        for copy in copies(k, new, True):
            copy.wait()


def update(layer, places, terms, total, weights, m, v, so_far):
    _, d, ff = weights[0].shape
    _, blocks, n, of_block, _ = weights[2].shape
    of_d, units = d // n, blocks // 2
    n_items = 2 * len(places)
    arrays = [*weights, *m, *v]
    aliased = list(so_far) if so_far is not None else []
    start = 1 + len(terms) + len(arrays)
    bytes_accessed = n_items * 11 * 3 * d * ff // n
    anywhere = pl.BlockSpec(memory_space=pl.ANY)
    return pl.pallas_call(
        functools.partial(update_kernel, n, layer, places, 3 * weights[0].size, len(terms)),
        in_specs=[pl.BlockSpec(memory_space=pltpu.VMEM)] + [anywhere] * (len(terms) + len(arrays) + len(aliased)),
        out_specs=[anywhere] * len(arrays),
        out_shape=[jax.ShapeDtypeStruct(one.shape, one.dtype) for one in arrays],
        scratch_shapes=[
            pltpu.VMEM((n_items, 2, of_d, ff // 2), BF16),
            pltpu.VMEM((n_items, units, of_block, d), BF16),
            pltpu.VMEM((n_items, 2, 2, of_d, ff // 2), F32),
            pltpu.VMEM((n_items, 2, units, of_block, d), F32),
            pltpu.VMEM((n_items, units, *terms[0].shape[-2:]), BF16),
            pltpu.SemaphoreType.DMA((n_items,)),
            pltpu.SemaphoreType.DMA((n_items,)),
        ],
        input_output_aliases={start + i: i for i in range(len(aliased))},
        compiler_params=pltpu.CompilerParams(vmem_limit_bytes=67_043_328),
        cost_estimate=pl.CostEstimate(flops=300 * bytes_accessed, bytes_accessed=bytes_accessed, transcendentals=0),
    )(total, *terms, *arrays, *aliased)


def solution(mesh):
    n = mesh.shape["dp"]
    half = n // 2

    def step(x, dy, *arrays):
        weights, m, v = (list(arrays[i : i + 3]) for i in (0, 3, 6))
        g1, g0a, g0b, total = reduced(n, x, dy, *weights)

        layers, ff, d = weights[2].shape
        split = (layers, ff // BLOCK, n, BLOCK // n, d)
        for group in (weights, m, v):
            group[2] = group[2].reshape(split)

        def sent(value, by):
            return lax.ppermute(value, "dp", [(i, (i + by) % n) for i in range(n)])

        rest = weights, m, v
        came = [[g0a, g0b]]
        right, left = (g0a, g0b), (g0a, g0b)
        for _ in range(1, half):
            a = sent(right[0], 1), sent(left[0], -1)
            b = sent(right[1], 1), sent(left[1], -1)
            right, left = (a[0], b[0]), (a[1], b[1])
            came.append([*right, *left])
        came.append([sent(right[0], 1), sent(left[1], -1)])

        jobs = [(1, list(range(k, k + n // 4)), [g1]) for k in range(0, n, n // 4)]
        jobs.append((0, [0, 1, n - 1], came[0] + came[1]))
        jobs += [(0, [k, n - k], came[k]) for k in range(2, half)]
        jobs.append((0, [half], came[half]))
        out = None
        for layer, places, terms in jobs:
            out = update(layer, places, terms, total, *rest, out)
        out = list(out)
        for i in (2, 5, 8):
            out[i] = out[i].reshape(layers, ff, d)
        return tuple(out)

    return jax.shard_map(
        step,
        mesh=mesh,
        in_specs=(P(("rep", "dp"), None, None),) * 2 + (P(None, None, None),) * 9,
        out_specs=(P("rep", None, None),) * 9,
        check_vma=False,
    )
```

```python
import functools

import jax
import jax.numpy as jnp
from jax import lax
from jax.experimental import pallas as pl
from jax.experimental.pallas import tpu as pltpu
from jax.sharding import PartitionSpec as P


BF16, F32 = jnp.bfloat16, jnp.float32
MESH = pl.DeviceIdType.MESH
LANES = 128
BLOCK, GATHERED = 256, 4
PLAIN, BY_ROWS = ((1,), (0,)), ((1,), (1,))


def dot(a, b, contract=PLAIN):
    return lax.dot_general(a, b, (contract, ((), ())), preferred_element_type=F32)


def scale_of(wide):
    return lax.rsqrt(jnp.mean(wide * wide, -1, keepdims=True) + 1e-6)


def normed(h):
    wide = h.astype(F32)
    return (wide * scale_of(wide)).astype(BF16)


def when(condition, do):
    if isinstance(condition, bool):
        if condition:
            do()
    else:
        pl.when(condition)(do)


def at_ring(e):
    return 5 * e // 2


def at_gather(e, half):
    return at_ring(half) + 2 + (5 * e if e < 2 else 3 * e + 3)


def main_kernel(
    n, x_hbm, dy_hbm, wg_hbm, wu_hbm, wd_hbm,
    g1_hbm, ga_ref, gb_ref, total_ref, a0t_hbm, h_hbm, dgu_hbm, gu_hbm,
    a, at, g, gt, wide, wgu, wd, acc_gu, acc_d, dgu, own, from_left, from_right, kept, squares, parts,
    x_sem, dy_sem, wide_sem, w_sem, dgu_sem, gu_sem, in_sem, send_sem, recv_sem, there_sem, here_sem, kept_sem, part_send, part_recv, credit,
):
    tokens, d = a.shape
    ff = wg_hbm.shape[2]
    block = wd.shape[1]
    blocks = ff // block
    units, half = 2 * blocks, n // 2
    tile = dgu.shape[1]
    tiles = tokens // tile
    small = tile // 2
    smalls = tokens // small
    chunk = small // 2
    chunks = tokens // chunk
    slots, shard_rows = own.shape[0], own.shape[2]
    gathered = kept.shape[0]
    me = lax.axis_index("dp")
    right, left = lax.rem(me + 1, n), lax.rem(me + n - 1, n)

    def span(i, size):
        return pl.ds(i * size, size) if isinstance(i, int) else pl.ds(pl.multiple_of(i * size, size), size)

    def dy_load(i):
        return pltpu.make_async_copy(dy_hbm.at[0, span(i, chunk)], g.at[span(i, chunk)], dy_sem.at[i])

    def wide_loads(layer):
        return [
            pltpu.make_async_copy(wg_hbm.at[layer], wide.at[:, pl.ds(0, ff)], wide_sem.at[0]),
            pltpu.make_async_copy(wu_hbm.at[layer], wide.at[:, pl.ds(ff, ff)], wide_sem.at[1]),
        ]

    def a0t_load(t):
        return pltpu.make_async_copy(a0t_hbm.at[:, span(t, tile)], at.at[:, span(t, tile)], in_sem.at[t])

    def gu_loads(b):
        slot = lax.rem(b, 2)
        return [
            pltpu.make_async_copy(ref.at[1, :, span(b, block)], wgu.at[slot, :, pl.ds(i * block, block)], w_sem.at[i, slot])
            for i, ref in enumerate((wg_hbm, wu_hbm))
        ]

    def down_load(b):
        last = jnp.int32(b < blocks) if isinstance(b, int) else (b < blocks).astype(jnp.int32)
        slot = lax.rem(b, 2)
        return pltpu.make_async_copy(wd_hbm.at[last, span(b - blocks * (1 - last), block), :], wd.at[slot], w_sem.at[2, slot])

    def ring_copy(u, k, way):
        slot = lax.rem(u, slots)
        ahead = half - k if way == 0 else n - half + k
        shard = lax.rem(me + ahead, n)
        rows = pl.ds(0, shard_rows)
        if k == 0:
            rows = pl.ds(way * (shard_rows // 2), shard_rows // 2)
        return pltpu.make_async_remote_copy(
            src_ref=own.at[slot, shard, rows],
            dst_ref=(from_left, from_right)[way].at[slot, k, rows],
            send_sem=send_sem.at[way, slot, k],
            recv_sem=recv_sem.at[way, slot, k],
            device_id={"dp": (right, left)[way]},
            device_id_type=MESH,
        )

    def ring_event(u, e, last):
        slot = lax.rem(u, slots)
        if e == 0:

            def take():
                pl.semaphore_wait(credit.at[0], 1)
                pl.semaphore_wait(credit.at[1], 1)

            when(u >= slots, take)
        else:
            for way in (0, 1):
                ring_copy(u, e - 1, way).wait()
        if 0 < e < half:
            for way in (0, 1):
                shard = lax.rem(me + (half - e if way == 0 else n - half + e), n)
                rows = pl.ds(0, shard_rows) if e > 1 else pl.ds(way * (shard_rows // 2), shard_rows // 2)
                came = (from_left, from_right)[way][slot, e - 1, rows].astype(F32)
                own[slot, shard, rows] = (own[slot, shard, rows].astype(F32) + came).astype(BF16)
        if e < half:
            for way in (0, 1):
                ring_copy(u, e, way).start()
        else:
            came = from_left[slot, e - 1].astype(F32) + from_right[slot, e - 1].astype(F32)
            done = (own[slot, me].astype(F32) + came).astype(BF16)

            def keep(ref, place):
                def do():
                    ref[jnp.clip(place, 0, ref.shape[0] - 1)] = done

                return do

            cut = gathered + ga_ref.shape[0]
            if last:
                when(u < gathered, keep(kept, u))
            when((u >= gathered) & (u < cut), keep(ga_ref, u - gathered))
            if not last:
                when(u >= cut, keep(gb_ref, u - cut))
            exact = done.astype(F32)
            squares[...] += jnp.sum((exact * exact).reshape(shard_rows // 8, 8, LANES), 0)

            def give():
                pl.semaphore_signal(credit.at[0], 1, device_id={"dp": left}, device_id_type=MESH)
                pl.semaphore_signal(credit.at[1], 1, device_id={"dp": right}, device_id_type=MESH)

            when(u < units - slots, give)

    def gather_copy(u, k, way):
        rows = pl.ds(0, shard_rows)
        if k == half - 1:
            rows = pl.ds(way * (shard_rows // 2), shard_rows // 2)
        place = (k, n - k)[way]
        after = (k + 1, n - k - 1)[way]
        return pltpu.make_async_remote_copy(
            src_ref=kept.at[u, rows] if k == 0 else g1_hbm.at[place, u, rows],
            dst_ref=g1_hbm.at[after, u, rows],
            send_sem=there_sem.at[way, u, k],
            recv_sem=here_sem.at[way, u, k],
            device_id={"dp": (right, left)[way]},
            device_id_type=MESH,
        )

    def kept_copy(u):
        return pltpu.make_async_copy(kept.at[u], g1_hbm.at[0, u], kept_sem.at[u])

    def gather_event(u, e):
        if e == 0:
            kept_copy(u).start()
        else:
            for way in (0, 1):
                gather_copy(u, e - 1, way).wait()
        if e < half:
            for way in (0, 1):
                gather_copy(u, e, way).start()
        else:
            kept_copy(u).wait()

    between = tiles * blocks
    second = between + smalls

    def events(now, phase):
        for last in (True, False):
            base, first = (0, 0) if last else (second, blocks)
            jobs = [(at_ring(e), blocks, functools.partial(ring_event, e=e, last=last)) for e in range(half + 1)]
            if last:
                jobs += [(at_gather(e, half), gathered, functools.partial(gather_event, e=e)) for e in range(half + 1)]
            for lag, count, job in jobs:
                earliest, latest = base + tiles + lag, base + tiles * count + lag
                lo, hi = ((0, between), (between, second), (second, second + between), (second + between, 1 << 30))[phase]
                if latest < lo or earliest >= hi:
                    continue
                since = now - earliest
                if isinstance(now, int):
                    if since >= 0 and since % tiles == 0 and since // tiles < count:
                        job(first + since // tiles)
                else:

                    @pl.when((since >= 0) & (lax.rem(since + 64 * tiles, tiles) == 0) & (since < tiles * count))
                    def _(job=job, since=since, first=first):
                        job(first + lax.div(since, tiles))

    def forward(x_in, a0t_out, h_out, z, gu_out, wd0):
        def x_load(i):
            slot = lax.rem(i, 4)
            return pltpu.make_async_copy(x_hbm.at[0, span(i, chunk)], x_in.at[slot], x_sem.at[slot])

        def first_stores(i):
            slot = lax.rem(i, 3)
            return [
                pltpu.make_async_copy(a0t_out.at[slot], a0t_hbm.at[:, span(i, chunk)], in_sem.at[slot]),
                pltpu.make_async_copy(gu_out.at[slot], gu_hbm.at[span(i, chunk)], gu_sem.at[slot]),
            ]

        def second_store(i):
            slot = lax.rem(i, 2)
            return pltpu.make_async_copy(h_out.at[slot], h_hbm.at[span(i, chunk)], dgu_sem.at[1, slot])

        def first(i):
            slot = lax.rem(i, 3)
            a0 = normed(x_in[lax.rem(i, 4)])
            a0t_out[slot] = a0.T
            cut = 2 * block
            for c in range(ff // cut):
                gate = dot(a0, wide[:, c * cut : (c + 1) * cut])
                up = dot(a0, wide[:, ff + c * cut : ff + (c + 1) * cut])
                gu_out[slot, :, pl.ds(c * cut, cut)] = gate
                gu_out[slot, :, pl.ds(ff + c * cut, cut)] = up
                z[lax.rem(i, 2), :, pl.ds(c * cut, cut)] = (gate * jax.nn.sigmoid(gate) * up).astype(BF16)

        def second(i):
            slot = lax.rem(i, 2)
            rows = span(i, chunk)
            h = (x_in[lax.rem(i, 4)].astype(F32) + dot(z[slot], wd0[...]).astype(BF16).astype(F32)).astype(BF16)
            h_out[slot] = h
            a1 = normed(h)
            a[rows] = a1
            at[:, rows] = a1.T
            gt[:, rows] = g[rows].T

        wd0_load = pltpu.make_async_copy(wd_hbm.at[0], wd0, wide_sem.at[2])
        x_load(0).start()
        for copy in wide_loads(0):
            copy.start()
        wd0_load.start()
        for i in (1, 2):
            x_load(i).start()
        for i in range(chunks):
            dy_load(i).start()
        for copy in gu_loads(0):
            copy.start()
        down_load(0).start()
        barrier = pltpu.get_barrier_semaphore()
        for k in range(1, n):
            pl.semaphore_signal(barrier, 1, device_id={"dp": lax.rem(me + k, n)}, device_id_type=MESH)
        squares[...] = jnp.zeros_like(squares)
        x_load(0).wait()
        for copy in wide_loads(0):
            copy.wait()
        first(0)
        for copy in first_stores(0):
            copy.start()
        wd0_load.wait()

        @pl.loop(1, chunks)
        def _(i):
            x_load(i).wait()
            dy_load(i - 1).wait()

            @pl.when(i >= 3)
            def _():
                for copy in first_stores(i - 3):
                    copy.wait()
                second_store(i - 3).wait()

            second(i - 1)
            first(i)
            for copy in first_stores(i):
                copy.start()
            second_store(i - 1).start()

            @pl.when(i + 2 < chunks)
            def _():
                x_load(i + 2).start()

        dy_load(chunks - 1).wait()
        second_store(chunks - 3).wait()
        second(chunks - 1)
        second_store(chunks - 1).start()
        for i in (chunks - 3, chunks - 2, chunks - 1):
            for copy in first_stores(i):
                copy.wait()
            if i >= chunks - 2:
                second_store(i).wait()
        pl.semaphore_wait(barrier, n - 1)

    def dgu_stores(b, t, slot):
        return [
            pltpu.make_async_copy(
                dgu.at[slot, :, pl.ds(i * block, block)],
                dgu_hbm.at[span(t, tile), pl.ds(pl.multiple_of(i * ff + b * block, block), block)],
                dgu_sem.at[i, slot],
            )
            for i in (0, 1)
        ]

    def steps(b, t, gu_in):
        rows = span(t, tile)
        slot = lax.rem(b, 2)
        gu = gu_in[lax.rem(t, 2)] if gu_in is not None else dot(a[rows], wgu[slot])
        dz = dot(g[rows], wd[slot], BY_ROWS).astype(BF16).astype(F32)
        gate, up = gu[:, :block], gu[:, block:]
        s = jax.nn.sigmoid(gate)
        silu = gate * s
        z = (silu * up).astype(BF16)
        dgate = (dz * up * (s + silu * (1 - s))).astype(BF16)
        dup = (dz * silu).astype(BF16)
        both = jnp.concatenate([dgate, dup], 1)
        if gu_in is None:
            dgu[lax.rem(t, 2)] = both
        acc_d[...] += dot(gt[:, rows], z)
        acc_gu[...] += dot(at[:, rows], both)

    def pack(b):
        slot = lax.rem(b, slots)
        of_d, of_block = d // n, block // n
        for s in range(n):
            for c in range(2 * block // LANES):
                piece = acc_gu[pl.ds(s * of_d, of_d), pl.ds(c * LANES, LANES)]
                own[slot, s, pl.ds(c * of_d, of_d)] = piece.astype(BF16)
        base = 2 * block // LANES * of_d
        for c in range(d // LANES):
            turned = acc_d[pl.ds(c * LANES, LANES)].T.astype(BF16)
            for s in range(n):
                own[slot, s, pl.ds(base + c * of_block, of_block)] = turned[s * of_block : (s + 1) * of_block]

    def clear():
        acc_gu[...] = jnp.zeros_like(acc_gu)
        acc_d[...] = jnp.zeros_like(acc_d)

    def last_block(b):
        @pl.when(b + 1 < blocks)
        def _():
            for copy in gu_loads(b + 1):
                copy.start()

        down_load(b + 1).start()
        for copy in gu_loads(b):
            copy.wait()
        down_load(b).wait()
        clear()

        @pl.loop(0, tiles)
        def _(t):
            @pl.when((b > 0) | (t > 1))
            def _():
                for copy in dgu_stores(b, t, lax.rem(t, 2)):
                    copy.wait()

            steps(b, t, None)
            for copy in dgu_stores(b, t, lax.rem(t, 2)):
                copy.start()
            events(b * tiles + t, 0)

        pack(b)

    def first_blocks(gu_in):
        def tile_loads(b, t):
            slot = lax.rem(t, 2)
            return [
                pltpu.make_async_copy(
                    gu_hbm.at[span(t, tile), pl.ds(pl.multiple_of(i * ff + (b - blocks) * block, block), block)],
                    gu_in.at[slot, :, pl.ds(i * block, block)],
                    dgu_sem.at[i, slot],
                )
                for i in (0, 1)
            ]

        for copy in tile_loads(blocks, 0):
            copy.start()

        @pl.loop(blocks, units)
        def _(b):
            @pl.when(b + 1 < units)
            def _():
                down_load(b + 1).start()

            down_load(b).wait()
            clear()

            @pl.loop(0, tiles)
            def _(t):
                @pl.when(b == blocks)
                def _():
                    a0t_load(t).wait()

                for copy in tile_loads(b, t):
                    copy.wait()
                ends = t == tiles - 1

                @pl.when((b + 1 < units) | jnp.logical_not(ends))
                def _():
                    for copy in tile_loads(jnp.where(ends, b + 1, b), jnp.where(ends, 0, t + 1)):
                        copy.start()

                steps(b, t, gu_in)
                events(second + (b - blocks) * tiles + t, 2)

            pack(b)

    def way_back(d_in, h_in):
        def in_loads(i, slot):
            return [
                pltpu.make_async_copy(dgu_hbm.at[span(i, small)], d_in.at[slot], dy_sem.at[slot]),
                pltpu.make_async_copy(h_hbm.at[span(i, small)], h_in.at[slot], dy_sem.at[2 + slot]),
            ]

        for copy in in_loads(0, 0):
            copy.start()
        for t in range(tiles):
            a0t_load(t).start()
        for copy in wide_loads(1):
            copy.wait()

        @pl.loop(0, smalls)
        def _(i):
            slot = lax.rem(i, 2)
            for copy in in_loads(i, slot):
                copy.wait()

            @pl.when(i + 1 < smalls)
            def _():
                for copy in in_loads(i + 1, 1 - slot):
                    copy.start()

            part = small // 2
            for c in range(2):
                here = pl.ds(c * part, part)
                rows = pl.ds(pl.multiple_of(i * small + c * part, part), part)
                by_a = dot(d_in[slot, here], wide[...], BY_ROWS).astype(BF16).astype(F32)
                h = h_in[slot, here].astype(F32)
                scale = scale_of(h)
                along = jnp.mean(by_a * h, -1, keepdims=True)
                by_h = (by_a * scale - h * (scale * scale * scale * along)).astype(BF16)
                out = (g[rows].astype(F32) + by_h.astype(F32)).astype(BF16)
                g[rows] = out
                gt[:, rows] = out.T
            events(between + i, 1)

    pl.run_scoped(
        forward,
        pltpu.VMEM((4, chunk, d), BF16),
        pltpu.VMEM((3, d, chunk), BF16),
        pltpu.VMEM((2, chunk, d), BF16),
        pltpu.VMEM((2, chunk, ff), BF16),
        pltpu.VMEM((3, chunk, 2 * ff), F32),
        pltpu.VMEM((ff, d), BF16),
    )
    for copy in wide_loads(1):
        copy.start()

    @pl.loop(0, blocks)
    def _(b):
        last_block(b)

    for t in (tiles - 2, tiles - 1):
        for copy in dgu_stores(blocks - 1, t, t % 2):
            copy.wait()
    pl.run_scoped(way_back, pltpu.VMEM((2, small, 2 * ff), BF16), pltpu.VMEM((2, small, d), BF16))
    pl.run_scoped(first_blocks, pltpu.VMEM((2, tile, 2 * block), F32))
    for now in range(second + between, second + between + at_ring(half) + 1):
        events(now, 3)

    def part_copy(k):
        return pltpu.make_async_remote_copy(
            src_ref=squares,
            dst_ref=parts.at[me],
            send_sem=part_send.at[k - 1],
            recv_sem=part_recv.at[k - 1],
            device_id={"dp": lax.rem(me + k, n)},
            device_id_type=MESH,
        )

    for k in range(1, n):
        part_copy(k).start()
    parts[me] = squares[...]
    for k in range(1, n):
        part_copy(k).wait()
    total = parts[0]
    for k in range(1, n):
        total = total + parts[k]
    total_ref[...] = total


def reduced(n, x, dy, w_gate, w_up, w_down):
    tokens, d = x.shape[1:]
    ff = w_gate.shape[2]
    block, tile = BLOCK, tokens // 4
    tiles, blocks, half = tokens // tile, ff // block, n // 2
    smalls = 2 * tiles
    shard_rows = 3 * d * block // (n * LANES)
    slots = at_ring(half) // tiles + 2
    anywhere, vmem = pl.BlockSpec(memory_space=pl.ANY), pl.BlockSpec(memory_space=pltpu.VMEM)
    dma = pltpu.SemaphoreType.DMA
    return pl.pallas_call(
        functools.partial(main_kernel, n),
        in_specs=[anywhere] * 5,
        out_specs=[anywhere, vmem, vmem, vmem] + [anywhere] * 4,
        out_shape=[
            jax.ShapeDtypeStruct((n, GATHERED, shard_rows, LANES), BF16),
            jax.ShapeDtypeStruct((blocks - GATHERED // 2, shard_rows, LANES), BF16),
            jax.ShapeDtypeStruct((blocks - GATHERED // 2, shard_rows, LANES), BF16),
            jax.ShapeDtypeStruct((8, LANES), F32),
            jax.ShapeDtypeStruct((d, tokens), BF16),
            jax.ShapeDtypeStruct((tokens, d), BF16),
            jax.ShapeDtypeStruct((tokens, 2 * ff), BF16),
            jax.ShapeDtypeStruct((tokens, 2 * ff), F32),
        ],
        scratch_shapes=[
            pltpu.VMEM((tokens, d), BF16),
            pltpu.VMEM((d, tokens), BF16),
            pltpu.VMEM((tokens, d), BF16),
            pltpu.VMEM((d, tokens), BF16),
            pltpu.VMEM((d, 2 * ff), BF16),
            pltpu.VMEM((2, d, 2 * block), BF16),
            pltpu.VMEM((2, block, d), BF16),
            pltpu.VMEM((d, 2 * block), F32),
            pltpu.VMEM((d, block), F32),
            pltpu.VMEM((2, tile, 2 * block), BF16),
            pltpu.VMEM((slots, n, shard_rows, LANES), BF16),
            pltpu.VMEM((slots, half, shard_rows, LANES), BF16),
            pltpu.VMEM((slots, half, shard_rows, LANES), BF16),
            pltpu.VMEM((GATHERED, shard_rows, LANES), BF16),
            pltpu.VMEM((8, LANES), F32),
            pltpu.VMEM((n, 8, LANES), F32),
            dma((4,)),
            dma((2 * smalls,)),
            dma((3,)),
            dma((3, 2)),
            dma((2, 2)),
            dma((3,)),
            dma((tiles,)),
            dma((2, slots, half)),
            dma((2, slots, half)),
            dma((2, GATHERED, half)),
            dma((2, GATHERED, half)),
            dma((GATHERED,)),
            dma((n - 1,)),
            dma((n - 1,)),
            pltpu.SemaphoreType.REGULAR((2,)),
        ],
        compiler_params=pltpu.CompilerParams(collective_id=0, has_side_effects=True, vmem_limit_bytes=67_043_328),
        cost_estimate=pl.CostEstimate(flops=34 * tokens * d * ff, bytes_accessed=16 * tokens * d, transcendentals=3 * tokens * ff),
        name="reduced",
    )(x, dy, w_gate, w_up, w_down)[:4]


def update_kernel(n, pieces, count, n_terms, *refs):
    total_ref, terms, (w, m, v) = refs[0], refs[1 : 1 + n_terms], (refs[1 + n_terms + 3 * i : 4 + n_terms + 3 * i] for i in range(3))
    *refs, flat_w, tall_w, flat, tall, grads, in_sem, out_sem = refs[10 + n_terms :]
    new = [refs[len(refs) - 9 + 3 * i : len(refs) - 6 + 3 * i] for i in range(3)]
    units = grads.shape[1]
    _, _, of_d, width = flat_w.shape
    of_block, d = tall_w.shape[2:]
    block = width // units
    slabs = block // LANES
    me = lax.axis_index("dp")

    def of(k, which):
        if isinstance(k, int):
            return pieces[k][which]
        found = jnp.int32(pieces[0][which])
        for i, piece in enumerate(pieces):
            if piece[which] != pieces[i - 1][which]:
                found = jnp.where(k >= i, piece[which], found)
        return found

    def copies(k, arrays, back):
        layer, pair, shard = of(k, 0), of(k, 1), lax.rem(me + n - of(k, 2), n)
        across = pl.ds(pl.multiple_of(shard * of_d, of_d), of_d), pl.ds(pl.multiple_of(pair * width, width), width)
        pairs = []
        for kind, (first, second, third) in enumerate(arrays):
            for i, ref in enumerate((first, second)):
                pairs.append((ref.at[layer, *across], flat_w.at[k, i] if kind == 0 else flat.at[k, kind - 1, i]))
            pairs.append((third.at[layer, pl.ds(pair * units, units), shard], tall_w.at[k] if kind == 0 else tall.at[k, kind - 1]))
        sem = out_sem.at[k] if back else in_sem.at[k]
        return [pltpu.make_async_copy(*(pair[::-1] if back else pair), sem) for pair in pairs]

    def term_copy(k):
        _, _, place, term, row = pieces[k]
        ref = terms[term]
        ref = ref.at[place, pl.ds(row, units)] if len(ref.shape) == 4 else ref.at[pl.ds(row, units)]
        return pltpu.make_async_copy(ref, grads.at[k], in_sem.at[k])

    ahead = min(2, len(pieces))
    for k in range(len(pieces)):
        term_copy(k).start()
        if k < ahead:
            for copy in copies(k, (w, m, v), False):
                copy.start()
    factor = jnp.minimum(1.0, 0.5 * lax.rsqrt(jnp.sum(total_ref[...], keepdims=True) / count + 1e-30))

    @pl.loop(0, len(pieces))
    def _(k):
        @pl.when(k + ahead < len(pieces))
        def _():
            for copy in copies(k + ahead, (w, m, v), False):
                copy.start()

        pltpu.make_async_copy(grads.at[k], grads.at[k], in_sem.at[k]).wait()
        for copy in copies(k, (w, m, v), False):
            copy.wait()

        def one(w_ref, m_ref, v_ref, where, term):
            term = term.astype(F32) * factor
            m_new = 0.9 * m_ref[where] + 0.1 * term
            v_new = 0.95 * v_ref[where] + 0.05 * term * term
            wide = w_ref[where].astype(F32)
            m_ref[where] = m_new
            v_ref[where] = v_new
            w_ref[where] = (wide - 0.02 * (m_new * lax.rsqrt(v_new + 1e-8) + 0.1 * wide)).astype(BF16)

        for j in range(units):
            for i in range(2):
                for c in range(slabs):
                    where = slice(None), pl.ds(j * block + c * LANES, LANES)
                    term = grads[k, j, pl.ds((i * slabs + c) * of_d, of_d)]
                    one(flat_w.at[k, i], flat.at[k, 0, i], flat.at[k, 1, i], where, term)
            for c in range(d // LANES):
                where = j, slice(None), pl.ds(c * LANES, LANES)
                term = grads[k, j, pl.ds(2 * slabs * of_d + c * of_block, of_block)]
                one(tall_w.at[k], tall.at[k, 0], tall.at[k, 1], where, term)
        for copy in copies(k, new, True):
            copy.start()

    @pl.loop(0, len(pieces))
    def _(k):
        for copy in copies(k, new, True):
            copy.wait()


def update(pieces, terms, total, weights, m, v, so_far):
    _, d, _ = weights[0].shape
    _, _, n, of_block, _ = weights[2].shape
    of_d, units, width, n_pieces = d // n, 2, 2 * BLOCK, len(pieces)
    arrays = [*weights, *m, *v]
    aliased = list(so_far) if so_far is not None else []
    start = 1 + len(terms) + len(arrays)
    bytes_accessed = n_pieces * 22 * 3 * d * width // n
    anywhere = pl.BlockSpec(memory_space=pl.ANY)
    return pl.pallas_call(
        functools.partial(update_kernel, n, pieces, 3 * weights[0].size, len(terms)),
        in_specs=[pl.BlockSpec(memory_space=pltpu.VMEM)] + [anywhere] * (len(terms) + len(arrays) + len(aliased)),
        out_specs=[anywhere] * len(arrays),
        out_shape=[jax.ShapeDtypeStruct(one.shape, one.dtype) for one in arrays],
        scratch_shapes=[
            pltpu.VMEM((n_pieces, 2, of_d, width), BF16),
            pltpu.VMEM((n_pieces, units, of_block, d), BF16),
            pltpu.VMEM((n_pieces, 2, 2, of_d, width), F32),
            pltpu.VMEM((n_pieces, 2, units, of_block, d), F32),
            pltpu.VMEM((n_pieces, units, *terms[0].shape[-2:]), BF16),
            pltpu.SemaphoreType.DMA((n_pieces,)),
            pltpu.SemaphoreType.DMA((n_pieces,)),
        ],
        input_output_aliases={start + i: i for i in range(len(aliased))},
        compiler_params=pltpu.CompilerParams(vmem_limit_bytes=67_043_328),
        cost_estimate=pl.CostEstimate(flops=300 * bytes_accessed, bytes_accessed=bytes_accessed, transcendentals=0),
        name="update",
    )(total, *terms, *arrays, *aliased)


def solution(mesh):
    n = mesh.shape["dp"]
    half = n // 2

    def step(x, dy, *arrays):
        weights, m, v = (list(arrays[i : i + 3]) for i in (0, 3, 6))
        g1, ga, gb, total = reduced(n, x, dy, *weights)

        layers, ff, d = weights[2].shape
        split = (layers, ff // BLOCK, n, BLOCK // n, d)
        for group in (weights, m, v):
            group[2] = group[2].reshape(split)

        def sent(value, by):
            return lax.ppermute(value, "dp", [(i, (i + by) % n) for i in range(n)])

        rest = weights, m, v
        pairs = ff // (2 * BLOCK)
        here = GATHERED // 2
        each = ga.shape[0] // 2
        came = {("a", 0): [(0, ga)], ("b", 0): [(0, gb)]}
        for k in range(1, half):
            for which in "ab":
                right, left = came[which, k - 1][0][1], came[which, k - 1][-1][1]
                came[which, k] = [(k, sent(right, 1)), (n - k, sent(left, -1))]
        came["a", half] = [(half, sent(came["a", half - 1][0][1], 1))]
        came["b", half] = [(half, sent(came["b", half - 1][1][1], -1))]

        jobs = [(range(0, 2), ["a0", "b0"]), (range(2, n - 2), []), (range(n - 2, n), ["a1"])]
        jobs += [((), [f"b{k - 1}", f"a{k}"] if k < 3 else [f"b{k - 1}"]) for k in range(2, half)]
        jobs += [((), [f"a{half - 1}"]), ((), [f"b{half - 1}"]), ((), [f"a{half}", f"b{half}"])]
        out = None
        for places, names in jobs:
            terms, pieces = [g1] if places else [], [(1, pair, place, 0, 2 * pair) for place in places for pair in range(here)]
            for name in names:
                for place, array in came[name[0], int(name[1:])]:
                    for i in range(each):
                        pair = here + i + (each if name[0] == "b" else 0)
                        pieces.append((1 if pair < pairs else 0, pair % pairs, place, len(terms), 2 * i))
                    terms.append(array)
            out = update(pieces, terms, total, *rest, out)
        out = list(out)
        for i in (2, 5, 8):
            out[i] = out[i].reshape(layers, ff, d)
        return tuple(out)

    return jax.shard_map(
        step,
        mesh=mesh,
        in_specs=(P(("rep", "dp"), None, None),) * 2 + (P(None, None, None),) * 9,
        out_specs=(P("rep", None, None),) * 9,
        check_vma=False,
    )
```

```python
import functools

import jax
import jax.numpy as jnp
from jax import lax
from jax.experimental import pallas as pl
from jax.experimental.pallas import tpu as pltpu
from jax.sharding import PartitionSpec as P


BF16, F32 = jnp.bfloat16, jnp.float32
MESH = pl.DeviceIdType.MESH
LANES = 128
BLOCK, GATHERED = 256, 4
PLAIN, BY_ROWS = ((1,), (0,)), ((1,), (1,))


def dot(a, b, contract=PLAIN):
    return lax.dot_general(a, b, (contract, ((), ())), preferred_element_type=F32)


def scale_of(wide):
    return lax.rsqrt(jnp.mean(wide * wide, -1, keepdims=True) + 1e-6)


def normed(h):
    wide = h.astype(F32)
    return (wide * scale_of(wide)).astype(BF16)


def when(condition, do):
    if isinstance(condition, bool):
        if condition:
            do()
    else:
        pl.when(condition)(do)


def at_ring(e, last):
    return 5 * e // 2 if last else 3 * e


def at_gather(e):
    return (13, 19, 25, 29, 32)[e] if e < 5 else 32 + 3 * (e - 4)


def main_kernel(
    n, x_hbm, dy_hbm, wg_hbm, wu_hbm, wd_hbm,
    g1_hbm, ga_hbm, gb_hbm, total_ref, a0t_hbm, h_hbm, dgu_hbm, gu_hbm,
    a, at, g, gt, wide, wgu, wd, acc_gu, acc_d, dgu, own, from_left, from_right, kept, squares, parts,
    x_sem, dy_sem, wide_sem, w_sem, dgu_sem, gu_sem, in_sem, send_sem, recv_sem, there_sem, here_sem, kept_sem, part_send, part_recv, credit,
):
    tokens, d = a.shape
    ff = wg_hbm.shape[2]
    block = wd.shape[1]
    blocks = ff // block
    units, half = 2 * blocks, n // 2
    tile = dgu.shape[1]
    tiles = tokens // tile
    small = tile // 2
    smalls = tokens // small
    chunk = small // 2
    chunks = tokens // chunk
    slots, shard_rows = own.shape[0], own.shape[2]
    gathered = g1_hbm.shape[1]
    me = lax.axis_index("dp")
    right, left = lax.rem(me + 1, n), lax.rem(me + n - 1, n)

    def span(i, size):
        return pl.ds(i * size, size) if isinstance(i, int) else pl.ds(pl.multiple_of(i * size, size), size)

    def dy_load(i):
        return pltpu.make_async_copy(dy_hbm.at[0, span(i, chunk)], g.at[span(i, chunk)], dy_sem.at[i])

    def wide_loads(layer):
        return [
            pltpu.make_async_copy(wg_hbm.at[layer], wide.at[:, pl.ds(0, ff)], wide_sem.at[0]),
            pltpu.make_async_copy(wu_hbm.at[layer], wide.at[:, pl.ds(ff, ff)], wide_sem.at[1]),
        ]

    def a0t_load(t):
        return pltpu.make_async_copy(a0t_hbm.at[:, span(t, tile)], at.at[:, span(t, tile)], in_sem.at[t])

    def gu_loads(b):
        slot = lax.rem(b, 2)
        return [
            pltpu.make_async_copy(ref.at[1, :, span(b, block)], wgu.at[slot, :, pl.ds(i * block, block)], w_sem.at[i, slot])
            for i, ref in enumerate((wg_hbm, wu_hbm))
        ]

    def down_load(b):
        last = jnp.int32(b < blocks) if isinstance(b, int) else (b < blocks).astype(jnp.int32)
        slot = lax.rem(b, 2)
        return pltpu.make_async_copy(wd_hbm.at[last, span(b - blocks * (1 - last), block), :], wd.at[slot], w_sem.at[2, slot])

    def ring_copy(u, k, way):
        slot = lax.rem(u, slots)
        ahead = half - k if way == 0 else n - half + k
        shard = lax.rem(me + ahead, n)
        rows = pl.ds(0, shard_rows)
        if k == 0:
            rows = pl.ds(way * (shard_rows // 2), shard_rows // 2)
        return pltpu.make_async_remote_copy(
            src_ref=own.at[slot, shard, rows],
            dst_ref=(from_left, from_right)[way].at[slot, k, rows],
            send_sem=send_sem.at[way, slot, k],
            recv_sem=recv_sem.at[way, slot, k],
            device_id={"dp": (right, left)[way]},
            device_id_type=MESH,
        )

    def ring_event(u, e, last):
        slot = lax.rem(u, slots)
        if e == 0:

            def take():
                pl.semaphore_wait(credit.at[0], 1)
                pl.semaphore_wait(credit.at[1], 1)

            when(u >= slots, take)
        else:
            for way in (0, 1):
                ring_copy(u, e - 1, way).wait()
        if 0 < e < half:
            for way in (0, 1):
                shard = lax.rem(me + (half - e if way == 0 else n - half + e), n)
                rows = pl.ds(0, shard_rows) if e > 1 else pl.ds(way * (shard_rows // 2), shard_rows // 2)
                came = (from_left, from_right)[way][slot, e - 1, rows].astype(F32)
                own[slot, shard, rows] = (own[slot, shard, rows].astype(F32) + came).astype(BF16)
        if e < half:
            for way in (0, 1):
                ring_copy(u, e, way).start()
        else:
            came = from_left[slot, e - 1].astype(F32) + from_right[slot, e - 1].astype(F32)
            done = (own[slot, me].astype(F32) + came).astype(BF16)
            kept[u] = done

            def hand_on(ref, place):
                return lambda: pltpu.make_async_copy(kept.at[u], ref.at[jnp.clip(place, 0, ref.shape[0] - 1)], kept_sem.at[u]).start()

            cut = gathered + ga_hbm.shape[0]
            when((u >= gathered) & (u < cut), hand_on(ga_hbm, u - gathered))
            if not last:
                when(u >= cut, hand_on(gb_hbm, u - cut))
            exact = done.astype(F32)
            squares[...] += jnp.sum((exact * exact).reshape(shard_rows // 8, 8, LANES), 0)

            def give():
                pl.semaphore_signal(credit.at[0], 1, device_id={"dp": left}, device_id_type=MESH)
                pl.semaphore_signal(credit.at[1], 1, device_id={"dp": right}, device_id_type=MESH)

            when(u < units - slots, give)

    def gather_copy(u, k, way):
        rows = pl.ds(0, shard_rows)
        if k == half - 1:
            rows = pl.ds(way * (shard_rows // 2), shard_rows // 2)
        place = (k, n - k)[way]
        after = (k + 1, n - k - 1)[way]
        return pltpu.make_async_remote_copy(
            src_ref=kept.at[u, rows] if k == 0 else g1_hbm.at[place, u, rows],
            dst_ref=g1_hbm.at[after, u, rows],
            send_sem=there_sem.at[way, u, k],
            recv_sem=here_sem.at[way, u, k],
            device_id={"dp": (right, left)[way]},
            device_id_type=MESH,
        )

    def kept_copy(u):
        return pltpu.make_async_copy(kept.at[u], g1_hbm.at[0, u], kept_sem.at[u])

    def gather_event(u, e):
        if e == 0:
            kept_copy(u).start()
        else:
            for way in (0, 1):
                gather_copy(u, e - 1, way).wait()
        if e < half:
            for way in (0, 1):
                gather_copy(u, e, way).start()
        else:
            kept_copy(u).wait()

    between = tiles * blocks
    second = between + smalls

    def events(now, phase, t=None):
        found = {}
        for last in (True, False):
            base, first = (0, 0) if last else (second, blocks)
            jobs = [(at_ring(e, last), blocks, functools.partial(ring_event, e=e, last=last)) for e in range(half + 1)]
            if last:
                jobs += [(at_gather(e), gathered, functools.partial(gather_event, e=e)) for e in range(half + 1)]
            for lag, count, job in jobs:
                earliest, latest = base + tiles + lag, base + tiles * count + lag
                lo, hi = ((0, between), (between, second), (second, second + between), (second + between, 1 << 30))[phase]
                if lo <= latest and earliest < hi:
                    found.setdefault(earliest % tiles, []).append((earliest, count, first, job))
        if isinstance(now, int):
            for earliest, count, first, job in found.get(now % tiles, []):
                if 0 <= now - earliest < tiles * count:
                    job(first + (now - earliest) // tiles)
            return
        for turn, some in found.items():

            @pl.when(t == turn)
            def _(some=some):
                for earliest, count, first, job in some:
                    since = now - earliest

                    @pl.when((since >= 0) & (since < tiles * count))
                    def _(job=job, since=since, first=first):
                        job(first + lax.div(since, tiles))

    def forward(x_in, a0t_out, h_out, z, gu_out, wd0):
        def x_load(i):
            slot = lax.rem(i, 4)
            return pltpu.make_async_copy(x_hbm.at[0, span(i, chunk)], x_in.at[slot], x_sem.at[slot])

        def first_stores(i):
            slot = lax.rem(i, 3)
            return [
                pltpu.make_async_copy(a0t_out.at[slot], a0t_hbm.at[:, span(i, chunk)], in_sem.at[slot]),
                pltpu.make_async_copy(gu_out.at[slot], gu_hbm.at[span(i, chunk)], gu_sem.at[slot]),
            ]

        def second_store(i):
            slot = lax.rem(i, 2)
            return pltpu.make_async_copy(h_out.at[slot], h_hbm.at[span(i, chunk)], dgu_sem.at[1, slot])

        def first(i):
            slot = lax.rem(i, 3)
            a0 = normed(x_in[lax.rem(i, 4)])
            a0t_out[slot] = a0.T
            cut = 2 * block
            for c in range(ff // cut):
                gate = dot(a0, wide[:, c * cut : (c + 1) * cut])
                up = dot(a0, wide[:, ff + c * cut : ff + (c + 1) * cut])
                gu_out[slot, :, pl.ds(c * cut, cut)] = gate
                gu_out[slot, :, pl.ds(ff + c * cut, cut)] = up
                z[lax.rem(i, 2), :, pl.ds(c * cut, cut)] = (gate * jax.nn.sigmoid(gate) * up).astype(BF16)

        def second(i):
            slot = lax.rem(i, 2)
            rows = span(i, chunk)
            h = (x_in[lax.rem(i, 4)].astype(F32) + dot(z[slot], wd0[...]).astype(BF16).astype(F32)).astype(BF16)
            h_out[slot] = h
            a1 = normed(h)
            a[rows] = a1
            at[:, rows] = a1.T
            gt[:, rows] = g[rows].T

        wd0_load = pltpu.make_async_copy(wd_hbm.at[0], wd0, wide_sem.at[2])
        x_load(0).start()
        for copy in wide_loads(0):
            copy.start()
        wd0_load.start()
        for i in (1, 2):
            x_load(i).start()
        for i in (0, 1, 2):
            dy_load(i).start()
        barrier = pltpu.get_barrier_semaphore()
        for k in range(1, n):
            pl.semaphore_signal(barrier, 1, device_id={"dp": lax.rem(me + k, n)}, device_id_type=MESH)
        squares[...] = jnp.zeros_like(squares)
        x_load(0).wait()
        for copy in wide_loads(0):
            copy.wait()
        first(0)
        for copy in first_stores(0):
            copy.start()
        wd0_load.wait()

        @pl.loop(1, chunks)
        def _(i):
            x_load(i).wait()
            dy_load(i - 1).wait()

            @pl.when(i >= 3)
            def _():
                for copy in first_stores(i - 3):
                    copy.wait()
                second_store(i - 3).wait()

            second(i - 1)
            first(i)
            for copy in first_stores(i):
                copy.start()
            second_store(i - 1).start()

            @pl.when(i + 2 < chunks)
            def _():
                dy_load(i + 2).start()
                x_load(i + 2).start()

            @pl.when(i == 1)
            def _():
                for copy in gu_loads(0):
                    copy.start()
                down_load(0).start()

        dy_load(chunks - 1).wait()
        second_store(chunks - 3).wait()
        second(chunks - 1)
        second_store(chunks - 1).start()
        for i in (chunks - 3, chunks - 2, chunks - 1):
            for copy in first_stores(i):
                copy.wait()
            if i >= chunks - 2:
                second_store(i).wait()
        pl.semaphore_wait(barrier, n - 1)

    def dgu_stores(b, t, slot):
        return [
            pltpu.make_async_copy(
                dgu.at[slot, :, pl.ds(i * block, block)],
                dgu_hbm.at[span(t, tile), pl.ds(pl.multiple_of(i * ff + b * block, block), block)],
                dgu_sem.at[i, slot],
            )
            for i in (0, 1)
        ]

    def steps(b, t, gu_in):
        rows = span(t, tile)
        slot = lax.rem(b, 2)
        gu = gu_in[lax.rem(t, 2)] if gu_in is not None else dot(a[rows], wgu[slot])
        dz = dot(g[rows], wd[slot], BY_ROWS).astype(BF16).astype(F32)
        gate, up = gu[:, :block], gu[:, block:]
        s = jax.nn.sigmoid(gate)
        silu = gate * s
        z = (silu * up).astype(BF16)
        dgate = (dz * up * (s + silu * (1 - s))).astype(BF16)
        dup = (dz * silu).astype(BF16)
        both = jnp.concatenate([dgate, dup], 1)
        if gu_in is None:
            dgu[lax.rem(t, 2)] = both
        acc_d[...] += dot(gt[:, rows], z)
        acc_gu[...] += dot(at[:, rows], both)

    def pack(b):
        slot = lax.rem(b, slots)
        of_d, of_block = d // n, block // n
        for s in range(n):
            for c in range(2 * block // LANES):
                piece = acc_gu[pl.ds(s * of_d, of_d), pl.ds(c * LANES, LANES)]
                own[slot, s, pl.ds(c * of_d, of_d)] = piece.astype(BF16)
        base = 2 * block // LANES * of_d
        for c in range(d // LANES):
            turned = acc_d[pl.ds(c * LANES, LANES)].T.astype(BF16)
            for s in range(n):
                own[slot, s, pl.ds(base + c * of_block, of_block)] = turned[s * of_block : (s + 1) * of_block]

    def clear():
        acc_gu[...] = jnp.zeros_like(acc_gu)
        acc_d[...] = jnp.zeros_like(acc_d)

    def last_block(b):
        @pl.when(b + 1 < blocks)
        def _():
            for copy in gu_loads(b + 1):
                copy.start()

        down_load(b + 1).start()
        for copy in gu_loads(b):
            copy.wait()
        down_load(b).wait()
        clear()

        @pl.loop(0, tiles)
        def _(t):
            @pl.when((b > 0) | (t > 1))
            def _():
                for copy in dgu_stores(b, t, lax.rem(t, 2)):
                    copy.wait()

            steps(b, t, None)
            for copy in dgu_stores(b, t, lax.rem(t, 2)):
                copy.start()
            events(b * tiles + t, 0, t)

        pack(b)

    def first_blocks(gu_in):
        def tile_loads(b, t):
            slot = lax.rem(t, 2)
            return [
                pltpu.make_async_copy(
                    gu_hbm.at[span(t, tile), pl.ds(pl.multiple_of(i * ff + (b - blocks) * block, block), block)],
                    gu_in.at[slot, :, pl.ds(i * block, block)],
                    dgu_sem.at[i, slot],
                )
                for i in (0, 1)
            ]

        for copy in tile_loads(blocks, 0):
            copy.start()

        @pl.loop(blocks, units)
        def _(b):
            @pl.when(b + 1 < units)
            def _():
                down_load(b + 1).start()

            down_load(b).wait()
            clear()

            @pl.loop(0, tiles)
            def _(t):
                @pl.when(b == blocks)
                def _():
                    a0t_load(t).wait()

                for copy in tile_loads(b, t):
                    copy.wait()
                ends = t == tiles - 1

                @pl.when((b + 1 < units) | jnp.logical_not(ends))
                def _():
                    for copy in tile_loads(jnp.where(ends, b + 1, b), jnp.where(ends, 0, t + 1)):
                        copy.start()

                steps(b, t, gu_in)
                events(second + (b - blocks) * tiles + t, 2, t)

            pack(b)

    def way_back(d_in, h_in):
        def in_loads(i, slot):
            return [
                pltpu.make_async_copy(dgu_hbm.at[span(i, small)], d_in.at[slot], dy_sem.at[slot]),
                pltpu.make_async_copy(h_hbm.at[span(i, small)], h_in.at[slot], dy_sem.at[2 + slot]),
            ]

        for copy in in_loads(0, 0):
            copy.start()
        for t in range(tiles):
            a0t_load(t).start()
        for copy in wide_loads(1):
            copy.wait()

        @pl.loop(0, smalls)
        def _(i):
            slot = lax.rem(i, 2)
            for copy in in_loads(i, slot):
                copy.wait()

            @pl.when(i + 1 < smalls)
            def _():
                for copy in in_loads(i + 1, 1 - slot):
                    copy.start()

            part = small // 2
            for c in range(2):
                here = pl.ds(c * part, part)
                rows = pl.ds(pl.multiple_of(i * small + c * part, part), part)
                by_a = dot(d_in[slot, here], wide[...], BY_ROWS).astype(BF16).astype(F32)
                h = h_in[slot, here].astype(F32)
                scale = scale_of(h)
                along = jnp.mean(by_a * h, -1, keepdims=True)
                by_h = (by_a * scale - h * (scale * scale * scale * along)).astype(BF16)
                out = (g[rows].astype(F32) + by_h.astype(F32)).astype(BF16)
                g[rows] = out
                gt[:, rows] = out.T
            events(between + i, 1, lax.rem(i, tiles))

    pl.run_scoped(
        forward,
        pltpu.VMEM((4, chunk, d), BF16),
        pltpu.VMEM((3, d, chunk), BF16),
        pltpu.VMEM((2, chunk, d), BF16),
        pltpu.VMEM((2, chunk, ff), BF16),
        pltpu.VMEM((3, chunk, 2 * ff), F32),
        pltpu.VMEM((ff, d), BF16),
    )
    for copy in wide_loads(1):
        copy.start()

    @pl.loop(0, blocks)
    def _(b):
        last_block(b)

    for t in (tiles - 2, tiles - 1):
        for copy in dgu_stores(blocks - 1, t, t % 2):
            copy.wait()
    pl.run_scoped(way_back, pltpu.VMEM((2, small, 2 * ff), BF16), pltpu.VMEM((2, small, d), BF16))
    pl.run_scoped(first_blocks, pltpu.VMEM((2, tile, 2 * block), F32))
    for now in range(second + between, second + between + at_ring(half, False) + 1):
        events(now, 3)

    def part_copy(k):
        return pltpu.make_async_remote_copy(
            src_ref=squares,
            dst_ref=parts.at[me],
            send_sem=part_send.at[k - 1],
            recv_sem=part_recv.at[k - 1],
            device_id={"dp": lax.rem(me + k, n)},
            device_id_type=MESH,
        )

    for k in range(1, n):
        part_copy(k).start()
    parts[me] = squares[...]
    for u in range(gathered, units):
        pltpu.make_async_copy(kept.at[u], ga_hbm.at[0], kept_sem.at[u]).wait()
    for k in range(1, n):
        part_copy(k).wait()
    total = parts[0]
    for k in range(1, n):
        total = total + parts[k]
    total_ref[...] = total


def reduced(n, x, dy, w_gate, w_up, w_down):
    tokens, d = x.shape[1:]
    ff = w_gate.shape[2]
    block, tile = BLOCK, tokens // 4
    tiles, blocks, half = tokens // tile, ff // block, n // 2
    smalls = 2 * tiles
    shard_rows = 3 * d * block // (n * LANES)
    slots = at_ring(half, False) // tiles + 1
    anywhere, vmem = pl.BlockSpec(memory_space=pl.ANY), pl.BlockSpec(memory_space=pltpu.VMEM)
    dma = pltpu.SemaphoreType.DMA
    return pl.pallas_call(
        functools.partial(main_kernel, n),
        in_specs=[anywhere] * 5,
        out_specs=[anywhere, anywhere, anywhere, vmem] + [anywhere] * 4,
        out_shape=[
            jax.ShapeDtypeStruct((n, GATHERED, shard_rows, LANES), BF16),
            jax.ShapeDtypeStruct((blocks - GATHERED // 2, shard_rows, LANES), BF16),
            jax.ShapeDtypeStruct((blocks - GATHERED // 2, shard_rows, LANES), BF16),
            jax.ShapeDtypeStruct((8, LANES), F32),
            jax.ShapeDtypeStruct((d, tokens), BF16),
            jax.ShapeDtypeStruct((tokens, d), BF16),
            jax.ShapeDtypeStruct((tokens, 2 * ff), BF16),
            jax.ShapeDtypeStruct((tokens, 2 * ff), F32),
        ],
        scratch_shapes=[
            pltpu.VMEM((tokens, d), BF16),
            pltpu.VMEM((d, tokens), BF16),
            pltpu.VMEM((tokens, d), BF16),
            pltpu.VMEM((d, tokens), BF16),
            pltpu.VMEM((d, 2 * ff), BF16),
            pltpu.VMEM((2, d, 2 * block), BF16),
            pltpu.VMEM((2, block, d), BF16),
            pltpu.VMEM((d, 2 * block), F32),
            pltpu.VMEM((d, block), F32),
            pltpu.VMEM((2, tile, 2 * block), BF16),
            pltpu.VMEM((slots, n, shard_rows, LANES), BF16),
            pltpu.VMEM((slots, half, shard_rows, LANES), BF16),
            pltpu.VMEM((slots, half, shard_rows, LANES), BF16),
            pltpu.VMEM((2 * blocks, shard_rows, LANES), BF16),
            pltpu.VMEM((8, LANES), F32),
            pltpu.VMEM((n, 8, LANES), F32),
            dma((4,)),
            dma((2 * smalls,)),
            dma((3,)),
            dma((3, 2)),
            dma((2, 2)),
            dma((3,)),
            dma((tiles,)),
            dma((2, slots, half)),
            dma((2, slots, half)),
            dma((2, GATHERED, half)),
            dma((2, GATHERED, half)),
            dma((2 * blocks,)),
            dma((n - 1,)),
            dma((n - 1,)),
            pltpu.SemaphoreType.REGULAR((2,)),
        ],
        compiler_params=pltpu.CompilerParams(collective_id=0, has_side_effects=True, vmem_limit_bytes=67_043_328),
        cost_estimate=pl.CostEstimate(flops=34 * tokens * d * ff, bytes_accessed=16 * tokens * d, transcendentals=3 * tokens * ff),
        name="reduced",
    )(x, dy, w_gate, w_up, w_down)[:4]


def update_kernel(n, pieces, count, n_terms, *refs):
    total_ref, terms, (w, m, v) = refs[0], refs[1 : 1 + n_terms], (refs[1 + n_terms + 3 * i : 4 + n_terms + 3 * i] for i in range(3))
    *refs, flat_w, tall_w, flat, tall, grads, in_sem, out_sem = refs[10 + n_terms :]
    new = [refs[len(refs) - 9 + 3 * i : len(refs) - 6 + 3 * i] for i in range(3)]
    units = grads.shape[1]
    _, _, of_d, width = flat_w.shape
    of_block, d = tall_w.shape[2:]
    block = width // units
    slabs = block // LANES
    me = lax.axis_index("dp")

    def of(k, which):
        if isinstance(k, int):
            return pieces[k][which]
        found = jnp.int32(pieces[0][which])
        for i, piece in enumerate(pieces):
            if piece[which] != pieces[i - 1][which]:
                found = jnp.where(k >= i, piece[which], found)
        return found

    def copies(k, arrays, back):
        layer, pair, shard = of(k, 0), of(k, 1), lax.rem(me + n - of(k, 2), n)
        across = pl.ds(pl.multiple_of(shard * of_d, of_d), of_d), pl.ds(pl.multiple_of(pair * width, width), width)
        pairs = []
        for kind, (first, second, third) in enumerate(arrays):
            for i, ref in enumerate((first, second)):
                pairs.append((ref.at[layer, *across], flat_w.at[k, i] if kind == 0 else flat.at[k, kind - 1, i]))
            pairs.append((third.at[layer, pl.ds(pair * units, units), shard], tall_w.at[k] if kind == 0 else tall.at[k, kind - 1]))
        sem = out_sem.at[k] if back else in_sem.at[k]
        return [pltpu.make_async_copy(*(pair[::-1] if back else pair), sem) for pair in pairs]

    def term_copy(k):
        _, _, place, term, row = pieces[k]
        ref = terms[term]
        ref = ref.at[place, pl.ds(row, units)] if len(ref.shape) == 4 else ref.at[pl.ds(row, units)]
        return pltpu.make_async_copy(ref, grads.at[k], in_sem.at[k])

    ahead = min(2, len(pieces))
    for k in range(len(pieces)):
        term_copy(k).start()
        if k < ahead:
            for copy in copies(k, (w, m, v), False):
                copy.start()
    factor = jnp.minimum(1.0, 0.5 * lax.rsqrt(jnp.sum(total_ref[...], keepdims=True) / count + 1e-30))

    @pl.loop(0, len(pieces))
    def _(k):
        @pl.when(k + ahead < len(pieces))
        def _():
            for copy in copies(k + ahead, (w, m, v), False):
                copy.start()

        pltpu.make_async_copy(grads.at[k], grads.at[k], in_sem.at[k]).wait()
        for copy in copies(k, (w, m, v), False):
            copy.wait()

        def one(w_ref, m_ref, v_ref, where, term):
            term = term.astype(F32) * factor
            m_new = 0.9 * m_ref[where] + 0.1 * term
            v_new = 0.95 * v_ref[where] + 0.05 * term * term
            wide = w_ref[where].astype(F32)
            m_ref[where] = m_new
            v_ref[where] = v_new
            w_ref[where] = (wide - 0.02 * (m_new * lax.rsqrt(v_new + 1e-8) + 0.1 * wide)).astype(BF16)

        for j in range(units):
            for i in range(2):
                for c in range(slabs):
                    where = slice(None), pl.ds(j * block + c * LANES, LANES)
                    term = grads[k, j, pl.ds((i * slabs + c) * of_d, of_d)]
                    one(flat_w.at[k, i], flat.at[k, 0, i], flat.at[k, 1, i], where, term)
            for c in range(d // LANES):
                where = j, slice(None), pl.ds(c * LANES, LANES)
                term = grads[k, j, pl.ds(2 * slabs * of_d + c * of_block, of_block)]
                one(tall_w.at[k], tall.at[k, 0], tall.at[k, 1], where, term)
        for copy in copies(k, new, True):
            copy.start()

    @pl.loop(0, len(pieces))
    def _(k):
        for copy in copies(k, new, True):
            copy.wait()


def update(pieces, terms, total, weights, m, v, so_far):
    _, d, _ = weights[0].shape
    _, _, n, of_block, _ = weights[2].shape
    of_d, units, width, n_pieces = d // n, 2, 2 * BLOCK, len(pieces)
    arrays = [*weights, *m, *v]
    aliased = list(so_far) if so_far is not None else []
    start = 1 + len(terms) + len(arrays)
    bytes_accessed = n_pieces * 22 * 3 * d * width // n
    anywhere = pl.BlockSpec(memory_space=pl.ANY)
    return pl.pallas_call(
        functools.partial(update_kernel, n, pieces, 3 * weights[0].size, len(terms)),
        in_specs=[pl.BlockSpec(memory_space=pltpu.VMEM)] + [anywhere] * (len(terms) + len(arrays) + len(aliased)),
        out_specs=[anywhere] * len(arrays),
        out_shape=[jax.ShapeDtypeStruct(one.shape, one.dtype) for one in arrays],
        scratch_shapes=[
            pltpu.VMEM((n_pieces, 2, of_d, width), BF16),
            pltpu.VMEM((n_pieces, units, of_block, d), BF16),
            pltpu.VMEM((n_pieces, 2, 2, of_d, width), F32),
            pltpu.VMEM((n_pieces, 2, units, of_block, d), F32),
            pltpu.VMEM((n_pieces, units, *terms[0].shape[-2:]), BF16),
            pltpu.SemaphoreType.DMA((n_pieces,)),
            pltpu.SemaphoreType.DMA((n_pieces,)),
        ],
        input_output_aliases={start + i: i for i in range(len(aliased))},
        compiler_params=pltpu.CompilerParams(vmem_limit_bytes=67_043_328),
        cost_estimate=pl.CostEstimate(flops=300 * bytes_accessed, bytes_accessed=bytes_accessed, transcendentals=0),
        name="update",
    )(total, *terms, *arrays, *aliased)


def solution(mesh):
    n = mesh.shape["dp"]
    half = n // 2

    def step(x, dy, *arrays):
        weights, m, v = (list(arrays[i : i + 3]) for i in (0, 3, 6))
        g1, ga, gb, total = reduced(n, x, dy, *weights)

        layers, ff, d = weights[2].shape
        split = (layers, ff // BLOCK, n, BLOCK // n, d)
        for group in (weights, m, v):
            group[2] = group[2].reshape(split)

        def sent(value, by):
            return lax.ppermute(value, "dp", [(i, (i + by) % n) for i in range(n)])

        rest = weights, m, v
        pairs = ff // (2 * BLOCK)
        here = GATHERED // 2
        each = ga.shape[0] // 2
        came = {("a", 0): [(0, ga)], ("b", 0): [(0, gb)]}
        for k in range(1, half):
            for which in "ab":
                right, left = came[which, k - 1][0][1], came[which, k - 1][-1][1]
                came[which, k] = [(k, sent(right, 1)), (n - k, sent(left, -1))]
        came["a", half] = [(half, sent(came["a", half - 1][0][1], 1))]
        came["b", half] = [(half, sent(came["b", half - 1][1][1], -1))]

        jobs = [(range(0, 2), ["a0", "b0"]), (range(2, n - 2), []), (range(n - 2, n), ["a1"])]
        jobs += [((), [f"b{k - 1}", f"a{k}"] if k < 3 else [f"b{k - 1}"]) for k in range(2, half)]
        jobs += [((), [f"a{half - 1}"]), ((), [f"b{half - 1}"]), ((), [f"a{half}", f"b{half}"])]
        out = None
        for places, names in jobs:
            terms, pieces = [g1] if places else [], [(1, pair, place, 0, 2 * pair) for place in places for pair in range(here)]
            for name in names:
                for place, array in came[name[0], int(name[1:])]:
                    for i in range(each):
                        pair = here + i + (each if name[0] == "b" else 0)
                        pieces.append((1 if pair < pairs else 0, pair % pairs, place, len(terms), 2 * i))
                    terms.append(array)
            out = update(pieces, terms, total, *rest, out)
        out = list(out)
        for i in (2, 5, 8):
            out[i] = out[i].reshape(layers, ff, d)
        return tuple(out)

    return jax.shard_map(
        step,
        mesh=mesh,
        in_specs=(P(("rep", "dp"), None, None),) * 2 + (P(None, None, None),) * 9,
        out_specs=(P("rep", None, None),) * 9,
        check_vma=False,
    )
```

```python
import functools

import jax
import jax.numpy as jnp
from jax import lax
from jax.experimental import pallas as pl
from jax.experimental.pallas import tpu as pltpu
from jax.sharding import PartitionSpec as P


BF16, F32 = jnp.bfloat16, jnp.float32
MESH = pl.DeviceIdType.MESH
LANES = 128
BLOCK, GATHERED = 256, 4
PLAIN, BY_ROWS = ((1,), (0,)), ((1,), (1,))


def dot(a, b, contract=PLAIN):
    return lax.dot_general(a, b, (contract, ((), ())), preferred_element_type=F32)


def scale_of(wide):
    return lax.rsqrt(jnp.mean(wide * wide, -1, keepdims=True) + 1e-6)


def normed(h):
    wide = h.astype(F32)
    return (wide * scale_of(wide)).astype(BF16)


def when(condition, do):
    if isinstance(condition, bool):
        if condition:
            do()
    else:
        pl.when(condition)(do)


def at_ring(e, last):
    return 5 * e // 2 if last else 3 * e


def at_gather(e):
    return (13, 19, 25, 29, 32)[e] if e < 5 else 32 + 3 * (e - 4)


def main_kernel(
    n, x_hbm, dy_hbm, wg_hbm, wu_hbm, wd_hbm,
    g1_hbm, ga_hbm, gb_hbm, right_hbm, left_hbm, total_ref, a0t_hbm, h_hbm, dgu_hbm, gu_hbm,
    a, at, g, gt, wide, wgu, wd, acc_gu, acc_d, dgu, own, from_left, from_right, kept, squares, parts,
    x_sem, dy_sem, wide_sem, w_sem, dgu_sem, gu_sem, in_sem, send_sem, recv_sem, there_sem, here_sem, kept_sem, go_sem, come_sem, part_send, part_recv, credit,
):
    tokens, d = a.shape
    ff = wg_hbm.shape[2]
    block = wd.shape[1]
    blocks = ff // block
    units, half = 2 * blocks, n // 2
    tile = dgu.shape[1]
    tiles = tokens // tile
    small = tile // 2
    smalls = tokens // small
    chunk = small // 2
    chunks = tokens // chunk
    slots, shard_rows = own.shape[0], own.shape[2]
    gathered = g1_hbm.shape[1]
    me = lax.axis_index("dp")
    right, left = lax.rem(me + 1, n), lax.rem(me + n - 1, n)

    def span(i, size):
        return pl.ds(i * size, size) if isinstance(i, int) else pl.ds(pl.multiple_of(i * size, size), size)

    def dy_load(i):
        return pltpu.make_async_copy(dy_hbm.at[0, span(i, chunk)], g.at[span(i, chunk)], dy_sem.at[i])

    def wide_loads(layer):
        return [
            pltpu.make_async_copy(wg_hbm.at[layer], wide.at[:, pl.ds(0, ff)], wide_sem.at[0]),
            pltpu.make_async_copy(wu_hbm.at[layer], wide.at[:, pl.ds(ff, ff)], wide_sem.at[1]),
        ]

    def a0t_load(t):
        return pltpu.make_async_copy(a0t_hbm.at[:, span(t, tile)], at.at[:, span(t, tile)], in_sem.at[t])

    def gu_loads(b):
        slot = lax.rem(b, 2)
        return [
            pltpu.make_async_copy(ref.at[1, :, span(b, block)], wgu.at[slot, :, pl.ds(i * block, block)], w_sem.at[i, slot])
            for i, ref in enumerate((wg_hbm, wu_hbm))
        ]

    def down_load(b):
        last = jnp.int32(b < blocks) if isinstance(b, int) else (b < blocks).astype(jnp.int32)
        slot = lax.rem(b, 2)
        return pltpu.make_async_copy(wd_hbm.at[last, span(b - blocks * (1 - last), block), :], wd.at[slot], w_sem.at[2, slot])

    def ring_copy(u, k, way):
        slot = lax.rem(u, slots)
        ahead = half - k if way == 0 else n - half + k
        shard = lax.rem(me + ahead, n)
        rows = pl.ds(0, shard_rows)
        if k == 0:
            rows = pl.ds(way * (shard_rows // 2), shard_rows // 2)
        return pltpu.make_async_remote_copy(
            src_ref=own.at[slot, shard, rows],
            dst_ref=(from_left, from_right)[way].at[slot, k, rows],
            send_sem=send_sem.at[way, slot, k],
            recv_sem=recv_sem.at[way, slot, k],
            device_id={"dp": (right, left)[way]},
            device_id_type=MESH,
        )

    def ring_event(u, e, last):
        slot = lax.rem(u, slots)
        if e == 0:

            def take():
                pl.semaphore_wait(credit.at[0], 1)
                pl.semaphore_wait(credit.at[1], 1)

            when(u >= slots, take)
        else:
            for way in (0, 1):
                ring_copy(u, e - 1, way).wait()
        if 0 < e < half:
            for way in (0, 1):
                shard = lax.rem(me + (half - e if way == 0 else n - half + e), n)
                rows = pl.ds(0, shard_rows) if e > 1 else pl.ds(way * (shard_rows // 2), shard_rows // 2)
                came = (from_left, from_right)[way][slot, e - 1, rows].astype(F32)
                own[slot, shard, rows] = (own[slot, shard, rows].astype(F32) + came).astype(BF16)
        if e < half:
            for way in (0, 1):
                ring_copy(u, e, way).start()
        else:
            came = from_left[slot, e - 1].astype(F32) + from_right[slot, e - 1].astype(F32)
            done = (own[slot, me].astype(F32) + came).astype(BF16)
            kept[u] = done

            def hand_on(ref, place):
                return lambda: pltpu.make_async_copy(kept.at[u], ref.at[jnp.clip(place, 0, ref.shape[0] - 1)], kept_sem.at[u]).start()

            cut = gathered + ga_hbm.shape[0]
            when((u >= gathered) & (u < cut), hand_on(ga_hbm, u - gathered))
            if not last:
                when(u >= cut, hand_on(gb_hbm, u - cut))
            exact = done.astype(F32)
            squares[...] += jnp.sum((exact * exact).reshape(shard_rows // 8, 8, LANES), 0)

            def give():
                pl.semaphore_signal(credit.at[0], 1, device_id={"dp": left}, device_id_type=MESH)
                pl.semaphore_signal(credit.at[1], 1, device_id={"dp": right}, device_id_type=MESH)

            when(u < units - slots, give)

    def gather_copy(u, k, way):
        rows = pl.ds(0, shard_rows)
        if k == half - 1:
            rows = pl.ds(way * (shard_rows // 2), shard_rows // 2)
        place = (k, n - k)[way]
        after = (k + 1, n - k - 1)[way]
        return pltpu.make_async_remote_copy(
            src_ref=kept.at[u, rows] if k == 0 else g1_hbm.at[place, u, rows],
            dst_ref=g1_hbm.at[after, u, rows],
            send_sem=there_sem.at[way, u, k],
            recv_sem=here_sem.at[way, u, k],
            device_id={"dp": (right, left)[way]},
            device_id_type=MESH,
        )

    def first_step(i):
        return [
            pltpu.make_async_remote_copy(
                src_ref=kept.at[gathered + i],
                dst_ref=(right_hbm, left_hbm)[way].at[i],
                send_sem=go_sem.at[way, i],
                recv_sem=come_sem.at[way, i],
                device_id={"dp": (right, left)[way]},
                device_id_type=MESH,
            )
            for way in (0, 1)
        ]

    def kept_copy(u):
        return pltpu.make_async_copy(kept.at[u], g1_hbm.at[0, u], kept_sem.at[u])

    def gather_event(u, e):
        if e == 0:
            kept_copy(u).start()
        else:
            for way in (0, 1):
                gather_copy(u, e - 1, way).wait()
        if e < half:
            for way in (0, 1):
                gather_copy(u, e, way).start()
        else:
            kept_copy(u).wait()

    between = tiles * blocks
    second = between + smalls

    def events(now, phase, t=None):
        found = {}
        for last in (True, False):
            base, first = (0, 0) if last else (second, blocks)
            jobs = [(at_ring(e, last), blocks, functools.partial(ring_event, e=e, last=last)) for e in range(half + 1)]
            if last:
                jobs += [(at_gather(e), gathered, functools.partial(gather_event, e=e)) for e in range(half + 1)]
            for lag, count, job in jobs:
                earliest, latest = base + tiles + lag, base + tiles * count + lag
                lo, hi = ((0, between), (between, second), (second, second + between), (second + between, 1 << 30))[phase]
                if lo <= latest and earliest < hi:
                    found.setdefault(earliest % tiles, []).append((earliest, count, first, job))
        if isinstance(now, int):
            for earliest, count, first, job in found.get(now % tiles, []):
                if 0 <= now - earliest < tiles * count:
                    job(first + (now - earliest) // tiles)
            return
        for turn, some in found.items():

            @pl.when(t == turn)
            def _(some=some):
                for earliest, count, first, job in some:
                    since = now - earliest

                    @pl.when((since >= 0) & (since < tiles * count))
                    def _(job=job, since=since, first=first):
                        job(first + lax.div(since, tiles))

    def forward(x_in, a0t_out, h_out, z, gu_out, wd0):
        def x_load(i):
            slot = lax.rem(i, 4)
            return pltpu.make_async_copy(x_hbm.at[0, span(i, chunk)], x_in.at[slot], x_sem.at[slot])

        def first_stores(i):
            slot = lax.rem(i, 3)
            return [
                pltpu.make_async_copy(a0t_out.at[slot], a0t_hbm.at[:, span(i, chunk)], in_sem.at[slot]),
                pltpu.make_async_copy(gu_out.at[slot], gu_hbm.at[span(i, chunk)], gu_sem.at[slot]),
            ]

        def second_store(i):
            slot = lax.rem(i, 2)
            return pltpu.make_async_copy(h_out.at[slot], h_hbm.at[span(i, chunk)], dgu_sem.at[1, slot])

        def first(i):
            slot = lax.rem(i, 3)
            a0 = normed(x_in[lax.rem(i, 4)])
            a0t_out[slot] = a0.T
            cut = 2 * block
            for c in range(ff // cut):
                gate = dot(a0, wide[:, c * cut : (c + 1) * cut])
                up = dot(a0, wide[:, ff + c * cut : ff + (c + 1) * cut])
                gu_out[slot, :, pl.ds(c * cut, cut)] = gate
                gu_out[slot, :, pl.ds(ff + c * cut, cut)] = up
                z[lax.rem(i, 2), :, pl.ds(c * cut, cut)] = (gate * jax.nn.sigmoid(gate) * up).astype(BF16)

        def second(i):
            slot = lax.rem(i, 2)
            rows = span(i, chunk)
            h = (x_in[lax.rem(i, 4)].astype(F32) + dot(z[slot], wd0[...]).astype(BF16).astype(F32)).astype(BF16)
            h_out[slot] = h
            a1 = normed(h)
            a[rows] = a1
            at[:, rows] = a1.T
            gt[:, rows] = g[rows].T

        wd0_load = pltpu.make_async_copy(wd_hbm.at[0], wd0, wide_sem.at[2])
        x_load(0).start()
        for copy in wide_loads(0):
            copy.start()
        wd0_load.start()
        for i in (1, 2):
            x_load(i).start()
        for i in (0, 1, 2):
            dy_load(i).start()
        barrier = pltpu.get_barrier_semaphore()
        for k in range(1, n):
            pl.semaphore_signal(barrier, 1, device_id={"dp": lax.rem(me + k, n)}, device_id_type=MESH)
        squares[...] = jnp.zeros_like(squares)
        x_load(0).wait()
        for copy in wide_loads(0):
            copy.wait()
        first(0)
        for copy in first_stores(0):
            copy.start()
        wd0_load.wait()

        @pl.loop(1, chunks)
        def _(i):
            x_load(i).wait()
            dy_load(i - 1).wait()

            @pl.when(i >= 3)
            def _():
                for copy in first_stores(i - 3):
                    copy.wait()
                second_store(i - 3).wait()

            second(i - 1)
            first(i)
            for copy in first_stores(i):
                copy.start()
            second_store(i - 1).start()

            @pl.when(i + 2 < chunks)
            def _():
                dy_load(i + 2).start()
                x_load(i + 2).start()

            @pl.when(i == 1)
            def _():
                for copy in gu_loads(0):
                    copy.start()
                down_load(0).start()

        dy_load(chunks - 1).wait()
        second_store(chunks - 3).wait()
        second(chunks - 1)
        second_store(chunks - 1).start()
        for i in (chunks - 3, chunks - 2, chunks - 1):
            for copy in first_stores(i):
                copy.wait()
            if i >= chunks - 2:
                second_store(i).wait()
        pl.semaphore_wait(barrier, n - 1)

    def dgu_stores(b, t, slot):
        return [
            pltpu.make_async_copy(
                dgu.at[slot, :, pl.ds(i * block, block)],
                dgu_hbm.at[span(t, tile), pl.ds(pl.multiple_of(i * ff + b * block, block), block)],
                dgu_sem.at[i, slot],
            )
            for i in (0, 1)
        ]

    def steps(b, t, gu_in):
        rows = span(t, tile)
        slot = lax.rem(b, 2)
        gu = gu_in[lax.rem(t, 2)] if gu_in is not None else dot(a[rows], wgu[slot])
        dz = dot(g[rows], wd[slot], BY_ROWS).astype(BF16).astype(F32)
        gate, up = gu[:, :block], gu[:, block:]
        s = jax.nn.sigmoid(gate)
        silu = gate * s
        z = (silu * up).astype(BF16)
        dgate = (dz * up * (s + silu * (1 - s))).astype(BF16)
        dup = (dz * silu).astype(BF16)
        both = jnp.concatenate([dgate, dup], 1)
        if gu_in is None:
            dgu[lax.rem(t, 2)] = both
        acc_d[...] += dot(gt[:, rows], z)
        acc_gu[...] += dot(at[:, rows], both)

    def pack(b):
        slot = lax.rem(b, slots)
        of_d, of_block = d // n, block // n
        for s in range(n):
            for c in range(2 * block // LANES):
                piece = acc_gu[pl.ds(s * of_d, of_d), pl.ds(c * LANES, LANES)]
                own[slot, s, pl.ds(c * of_d, of_d)] = piece.astype(BF16)
        base = 2 * block // LANES * of_d
        for c in range(d // LANES):
            turned = acc_d[pl.ds(c * LANES, LANES)].T.astype(BF16)
            for s in range(n):
                own[slot, s, pl.ds(base + c * of_block, of_block)] = turned[s * of_block : (s + 1) * of_block]

    def clear():
        acc_gu[...] = jnp.zeros_like(acc_gu)
        acc_d[...] = jnp.zeros_like(acc_d)

    def last_block(b):
        @pl.when(b + 1 < blocks)
        def _():
            for copy in gu_loads(b + 1):
                copy.start()

        down_load(b + 1).start()
        for copy in gu_loads(b):
            copy.wait()
        down_load(b).wait()
        clear()

        @pl.loop(0, tiles)
        def _(t):
            @pl.when((b > 0) | (t > 1))
            def _():
                for copy in dgu_stores(b, t, lax.rem(t, 2)):
                    copy.wait()

            steps(b, t, None)
            for copy in dgu_stores(b, t, lax.rem(t, 2)):
                copy.start()
            events(b * tiles + t, 0, t)

        pack(b)

    def first_blocks(gu_in):
        def tile_loads(b, t):
            slot = lax.rem(t, 2)
            return [
                pltpu.make_async_copy(
                    gu_hbm.at[span(t, tile), pl.ds(pl.multiple_of(i * ff + (b - blocks) * block, block), block)],
                    gu_in.at[slot, :, pl.ds(i * block, block)],
                    dgu_sem.at[i, slot],
                )
                for i in (0, 1)
            ]

        for copy in tile_loads(blocks, 0):
            copy.start()

        @pl.loop(blocks, units)
        def _(b):
            @pl.when(b + 1 < units)
            def _():
                down_load(b + 1).start()

            down_load(b).wait()
            clear()

            @pl.loop(0, tiles)
            def _(t):
                @pl.when(b == blocks)
                def _():
                    a0t_load(t).wait()

                for copy in tile_loads(b, t):
                    copy.wait()
                ends = t == tiles - 1

                @pl.when((b + 1 < units) | jnp.logical_not(ends))
                def _():
                    for copy in tile_loads(jnp.where(ends, b + 1, b), jnp.where(ends, 0, t + 1)):
                        copy.start()

                steps(b, t, gu_in)
                events(second + (b - blocks) * tiles + t, 2, t)

            pack(b)

    def way_back(d_in, h_in):
        def in_loads(i, slot):
            return [
                pltpu.make_async_copy(dgu_hbm.at[span(i, small)], d_in.at[slot], dy_sem.at[slot]),
                pltpu.make_async_copy(h_hbm.at[span(i, small)], h_in.at[slot], dy_sem.at[2 + slot]),
            ]

        for copy in in_loads(0, 0):
            copy.start()
        for t in range(tiles):
            a0t_load(t).start()
        for copy in wide_loads(1):
            copy.wait()

        @pl.loop(0, smalls)
        def _(i):
            slot = lax.rem(i, 2)
            for copy in in_loads(i, slot):
                copy.wait()

            @pl.when(i + 1 < smalls)
            def _():
                for copy in in_loads(i + 1, 1 - slot):
                    copy.start()

            part = small // 2
            for c in range(2):
                here = pl.ds(c * part, part)
                rows = pl.ds(pl.multiple_of(i * small + c * part, part), part)
                by_a = dot(d_in[slot, here], wide[...], BY_ROWS).astype(BF16).astype(F32)
                h = h_in[slot, here].astype(F32)
                scale = scale_of(h)
                along = jnp.mean(by_a * h, -1, keepdims=True)
                by_h = (by_a * scale - h * (scale * scale * scale * along)).astype(BF16)
                out = (g[rows].astype(F32) + by_h.astype(F32)).astype(BF16)
                g[rows] = out
                gt[:, rows] = out.T
            events(between + i, 1, lax.rem(i, tiles))

    pl.run_scoped(
        forward,
        pltpu.VMEM((4, chunk, d), BF16),
        pltpu.VMEM((3, d, chunk), BF16),
        pltpu.VMEM((2, chunk, d), BF16),
        pltpu.VMEM((2, chunk, ff), BF16),
        pltpu.VMEM((3, chunk, 2 * ff), F32),
        pltpu.VMEM((ff, d), BF16),
    )
    for copy in wide_loads(1):
        copy.start()

    @pl.loop(0, blocks)
    def _(b):
        last_block(b)

    for t in (tiles - 2, tiles - 1):
        for copy in dgu_stores(blocks - 1, t, t % 2):
            copy.wait()
    pl.run_scoped(way_back, pltpu.VMEM((2, small, 2 * ff), BF16), pltpu.VMEM((2, small, d), BF16))
    pl.run_scoped(first_blocks, pltpu.VMEM((2, tile, 2 * block), F32))
    ends, early = second + between, {at_ring(half - 2, False): 0, at_ring(half - 1, False): 1}
    for since in range(at_ring(half, False) + 1):
        events(ends + since, 3)
        if since in early:
            for copy in first_step(early[since]):
                copy.start()

    def part_copy(k):
        return pltpu.make_async_remote_copy(
            src_ref=squares,
            dst_ref=parts.at[me],
            send_sem=part_send.at[k - 1],
            recv_sem=part_recv.at[k - 1],
            device_id={"dp": lax.rem(me + k, n)},
            device_id_type=MESH,
        )

    for k in range(1, n):
        part_copy(k).start()
    for i in range(2, ga_hbm.shape[0]):
        for copy in first_step(i):
            copy.start()
    parts[me] = squares[...]
    for u in range(gathered, units):
        pltpu.make_async_copy(kept.at[u], ga_hbm.at[0], kept_sem.at[u]).wait()
    for k in range(1, n):
        part_copy(k).wait()
    total = parts[0]
    for k in range(1, n):
        total = total + parts[k]
    total_ref[...] = total
    for i in range(ga_hbm.shape[0]):
        for copy in first_step(i):
            copy.wait()


def reduced(n, x, dy, w_gate, w_up, w_down):
    tokens, d = x.shape[1:]
    ff = w_gate.shape[2]
    block, tile = BLOCK, tokens // 4
    tiles, blocks, half = tokens // tile, ff // block, n // 2
    smalls = 2 * tiles
    shard_rows = 3 * d * block // (n * LANES)
    slots = at_ring(half, False) // tiles + 1
    anywhere, vmem = pl.BlockSpec(memory_space=pl.ANY), pl.BlockSpec(memory_space=pltpu.VMEM)
    dma = pltpu.SemaphoreType.DMA
    return pl.pallas_call(
        functools.partial(main_kernel, n),
        in_specs=[anywhere] * 5,
        out_specs=[anywhere] * 5 + [vmem] + [anywhere] * 4,
        out_shape=[
            jax.ShapeDtypeStruct((n, GATHERED, shard_rows, LANES), BF16),
            *[jax.ShapeDtypeStruct((blocks - GATHERED // 2, shard_rows, LANES), BF16)] * 4,
            jax.ShapeDtypeStruct((8, LANES), F32),
            jax.ShapeDtypeStruct((d, tokens), BF16),
            jax.ShapeDtypeStruct((tokens, d), BF16),
            jax.ShapeDtypeStruct((tokens, 2 * ff), BF16),
            jax.ShapeDtypeStruct((tokens, 2 * ff), F32),
        ],
        scratch_shapes=[
            pltpu.VMEM((tokens, d), BF16),
            pltpu.VMEM((d, tokens), BF16),
            pltpu.VMEM((tokens, d), BF16),
            pltpu.VMEM((d, tokens), BF16),
            pltpu.VMEM((d, 2 * ff), BF16),
            pltpu.VMEM((2, d, 2 * block), BF16),
            pltpu.VMEM((2, block, d), BF16),
            pltpu.VMEM((d, 2 * block), F32),
            pltpu.VMEM((d, block), F32),
            pltpu.VMEM((2, tile, 2 * block), BF16),
            pltpu.VMEM((slots, n, shard_rows, LANES), BF16),
            pltpu.VMEM((slots, half, shard_rows, LANES), BF16),
            pltpu.VMEM((slots, half, shard_rows, LANES), BF16),
            pltpu.VMEM((2 * blocks, shard_rows, LANES), BF16),
            pltpu.VMEM((8, LANES), F32),
            pltpu.VMEM((n, 8, LANES), F32),
            dma((4,)),
            dma((2 * smalls,)),
            dma((3,)),
            dma((3, 2)),
            dma((2, 2)),
            dma((3,)),
            dma((tiles,)),
            dma((2, slots, half)),
            dma((2, slots, half)),
            dma((2, GATHERED, half)),
            dma((2, GATHERED, half)),
            dma((2 * blocks,)),
            *[dma((2, blocks - GATHERED // 2))] * 2,
            dma((n - 1,)),
            dma((n - 1,)),
            pltpu.SemaphoreType.REGULAR((2,)),
        ],
        compiler_params=pltpu.CompilerParams(collective_id=0, has_side_effects=True, vmem_limit_bytes=67_043_328),
        cost_estimate=pl.CostEstimate(flops=34 * tokens * d * ff, bytes_accessed=16 * tokens * d, transcendentals=3 * tokens * ff),
        name="reduced",
    )(x, dy, w_gate, w_up, w_down)[:6]


def update_kernel(n, pieces, count, n_terms, *refs):
    total_ref, terms, (w, m, v) = refs[0], refs[1 : 1 + n_terms], (refs[1 + n_terms + 3 * i : 4 + n_terms + 3 * i] for i in range(3))
    *refs, flat_w, tall_w, flat, tall, grads, squares, in_sem, out_sem = refs[10 + n_terms :]
    new = [refs[len(refs) - 9 + 3 * i : len(refs) - 6 + 3 * i] for i in range(3)]
    units = grads.shape[1]
    _, _, of_d, width = flat_w.shape
    of_block, d = tall_w.shape[2:]
    block = width // units
    slabs = block // LANES
    me = lax.axis_index("dp")

    def of(k, which):
        if isinstance(k, int):
            return pieces[k][which]
        found = jnp.int32(pieces[0][which])
        for i, piece in enumerate(pieces):
            if piece[which] != pieces[i - 1][which]:
                found = jnp.where(k >= i, piece[which], found)
        return found

    def copies(k, arrays, back):
        layer, pair, shard = of(k, 0), of(k, 1), lax.rem(me + n - of(k, 2), n)
        across = pl.ds(pl.multiple_of(shard * of_d, of_d), of_d), pl.ds(pl.multiple_of(pair * width, width), width)
        pairs = []
        for kind, (first, second, third) in enumerate(arrays):
            for i, ref in enumerate((first, second)):
                pairs.append((ref.at[layer, *across], flat_w.at[k, i] if kind == 0 else flat.at[k, kind - 1, i]))
            pairs.append((third.at[layer, pl.ds(pair * units, units), shard], tall_w.at[k] if kind == 0 else tall.at[k, kind - 1]))
        sem = out_sem.at[k] if back else in_sem.at[k]
        return [pltpu.make_async_copy(*(pair[::-1] if back else pair), sem) for pair in pairs]

    def term_copy(k):
        _, _, place, term, row = pieces[k]
        ref = terms[term]
        ref = ref.at[place, pl.ds(row, units)] if len(ref.shape) == 4 else ref.at[pl.ds(row, units)]
        return pltpu.make_async_copy(ref, grads.at[k], in_sem.at[k])

    ahead = min(2, len(pieces))
    total_copy = pltpu.make_async_copy(total_ref, squares, out_sem.at[0])
    total_copy.start()
    for k in range(len(pieces)):
        term_copy(k).start()
        if k < ahead:
            for copy in copies(k, (w, m, v), False):
                copy.start()
    total_copy.wait()
    factor = jnp.minimum(1.0, 0.5 * lax.rsqrt(jnp.sum(squares[...], keepdims=True) / count + 1e-30))

    @pl.loop(0, len(pieces))
    def _(k):
        @pl.when(k + ahead < len(pieces))
        def _():
            for copy in copies(k + ahead, (w, m, v), False):
                copy.start()

        pltpu.make_async_copy(grads.at[k], grads.at[k], in_sem.at[k]).wait()
        for copy in copies(k, (w, m, v), False):
            copy.wait()

        def one(w_ref, m_ref, v_ref, where, term):
            term = term.astype(F32) * factor
            m_new = 0.9 * m_ref[where] + 0.1 * term
            v_new = 0.95 * v_ref[where] + 0.05 * term * term
            wide = w_ref[where].astype(F32)
            m_ref[where] = m_new
            v_ref[where] = v_new
            w_ref[where] = (wide - 0.02 * (m_new * lax.rsqrt(v_new + 1e-8) + 0.1 * wide)).astype(BF16)

        for j in range(units):
            for i in range(2):
                for c in range(slabs):
                    where = slice(None), pl.ds(j * block + c * LANES, LANES)
                    term = grads[k, j, pl.ds((i * slabs + c) * of_d, of_d)]
                    one(flat_w.at[k, i], flat.at[k, 0, i], flat.at[k, 1, i], where, term)
            for c in range(d // LANES):
                where = j, slice(None), pl.ds(c * LANES, LANES)
                term = grads[k, j, pl.ds(2 * slabs * of_d + c * of_block, of_block)]
                one(tall_w.at[k], tall.at[k, 0], tall.at[k, 1], where, term)
        for copy in copies(k, new, True):
            copy.start()

    @pl.loop(0, len(pieces))
    def _(k):
        for copy in copies(k, new, True):
            copy.wait()


def update(pieces, terms, total, weights, m, v, so_far):
    _, d, _ = weights[0].shape
    _, _, n, of_block, _ = weights[2].shape
    of_d, units, width, n_pieces = d // n, 2, 2 * BLOCK, len(pieces)
    arrays = [*weights, *m, *v]
    aliased = list(so_far) if so_far is not None else []
    start = 1 + len(terms) + len(arrays)
    bytes_accessed = n_pieces * 22 * 3 * d * width // n
    anywhere = pl.BlockSpec(memory_space=pl.ANY)
    return pl.pallas_call(
        functools.partial(update_kernel, n, pieces, 3 * weights[0].size, len(terms)),
        in_specs=[anywhere] * (1 + len(terms) + len(arrays) + len(aliased)),
        out_specs=[anywhere] * len(arrays),
        out_shape=[jax.ShapeDtypeStruct(one.shape, one.dtype) for one in arrays],
        scratch_shapes=[
            pltpu.VMEM((n_pieces, 2, of_d, width), BF16),
            pltpu.VMEM((n_pieces, units, of_block, d), BF16),
            pltpu.VMEM((n_pieces, 2, 2, of_d, width), F32),
            pltpu.VMEM((n_pieces, 2, units, of_block, d), F32),
            pltpu.VMEM((n_pieces, units, *terms[0].shape[-2:]), BF16),
            pltpu.VMEM(total.shape, F32),
            pltpu.SemaphoreType.DMA((n_pieces,)),
            pltpu.SemaphoreType.DMA((n_pieces,)),
        ],
        input_output_aliases={start + i: i for i in range(len(aliased))},
        compiler_params=pltpu.CompilerParams(vmem_limit_bytes=67_043_328),
        cost_estimate=pl.CostEstimate(flops=300 * bytes_accessed, bytes_accessed=bytes_accessed, transcendentals=0),
        name="update",
    )(total, *terms, *arrays, *aliased)


def solution(mesh):
    n = mesh.shape["dp"]
    half = n // 2
    sends = [one for k in range(1, half) for one in (("a", k + 1), ("b", k))] + [("b", half)]

    def ways(which, k):
        return ("right", "left") if k < half else ("right",) if which == "a" else ("left",)

    def step(x, dy, *arrays):
        weights, m, v = (list(arrays[i : i + 3]) for i in (0, 3, 6))
        g1, ga, gb, ga_right, ga_left, total = reduced(n, x, dy, *weights)

        layers, ff, d = weights[2].shape
        split = (layers, ff // BLOCK, n, BLOCK // n, d)
        for group in (weights, m, v):
            group[2] = group[2].reshape(split)

        def sent(value, by):
            return lax.ppermute(value, "dp", [(i, (i + by) % n) for i in range(n)])

        rest = weights, m, v
        pairs = ff // (2 * BLOCK)
        here = GATHERED // 2
        each = ga.shape[0] // 2
        came = {("a", 0): [(0, ga)], ("b", 0): [(0, gb)], ("a", 1): [(1, ga_right), (n - 1, ga_left)]}
        for which, k in sends:
            right, left = came[which, k - 1][0][1], came[which, k - 1][-1][1]
            came[which, k] = [
                (k if by > 0 else n - k, sent(one, by))
                for one, by, way in ((right, 1, "right"), (left, -1, "left"))
                if way in ways(which, k)
            ]

        jobs = [(range(0, 1), ["a0", "b0", "a1"]), (range(1, half + 1), []), (range(half + 1, n), [])]
        jobs += [((), [f"{which}{k}" for which, k in sends[2 * i : 2 * i + 2]]) for i in range(half - 2)]
        jobs += [((), [f"b{half - 1}", f"a{half}"]), ((), [f"b{half}"])]
        out = None
        for places, names in jobs:
            terms, pieces = [g1] if places else [], [(1, pair, place, 0, 2 * pair) for place in places for pair in range(here)]
            for name in names:
                for place, array in came[name[0], int(name[1:])]:
                    for i in range(each):
                        pair = here + i + (each if name[0] == "b" else 0)
                        pieces.append((1 if pair < pairs else 0, pair % pairs, place, len(terms), 2 * i))
                    terms.append(array)
            out = update(pieces, terms, total, *rest, out)
        out = list(out)
        for i in (2, 5, 8):
            out[i] = out[i].reshape(layers, ff, d)
        return tuple(out)

    return jax.shard_map(
        step,
        mesh=mesh,
        in_specs=(P(("rep", "dp"), None, None),) * 2 + (P(None, None, None),) * 9,
        out_specs=(P("rep", None, None),) * 9,
        check_vma=False,
    )
```
